32 devices in a mesh: dp: 4 (over y, z), sp: 8 (over x, core).
Axes of the slice: x: 4, y: 2, z: 2, core: 2. Of those that a mesh axis runs over, the one named last changes fastest.
The devices are a block of a 4x4x8 slice.
Arguments:
- signal: bfloat16 [262144, 256], P(('dp', 'sp')), parts along dimension 0
- w_first: bfloat16 [11, 2048, 2, 32, 32], P(None, 'sp')
- w_second: bfloat16 [11, 2048, 2, 32, 32], P(None, 'sp')
Outputs:
- output: bfloat16 [262144, 256], P(('dp', 'sp')), parts along dimension 0
There are 4 independent parts. The reference program is written for one: setup_inputs(seed, part) draws one part's arguments, and reference() takes and returns one part's arrays. A program takes and returns all parts, laid end to end along the dimension named above; an argument that names none is the same for every part.
All inputs are finite; a program needn't handle non-finite values.
Results may differ from the reference program's by a relative error of at most 0.02.
Values are sent between devices in bfloat16 or wider.
A program may use at most 768 MiB of HBM per device.

```python
import jax
import jax.numpy as jnp
import math
from jax import lax

SEQ_LEN = 65536
CHANNELS = 256
BLOCK_SIZE = 32

NUM_BLOCKS = SEQ_LEN // BLOCK_SIZE
STAGES = int(math.log2(NUM_BLOCKS))


def setup_inputs(seed: int = 0, part: int = 0) -> dict:
    key_signal = jax.random.fold_in(jax.random.key(seed + 1), part)
    key_first = jax.random.key(seed + 2)
    key_second = jax.random.key(seed + 3)
    w_shape = (STAGES, NUM_BLOCKS, 2, BLOCK_SIZE, BLOCK_SIZE)
    w_scale = (2 * BLOCK_SIZE) ** -0.5
    signal = jax.random.normal(key_signal, (SEQ_LEN, CHANNELS), jnp.float32)
    w_first = jax.random.normal(key_first, w_shape, jnp.float32) * w_scale
    w_second = jax.random.normal(key_second, w_shape, jnp.float32) * w_scale
    return {"signal": signal.astype(jnp.bfloat16), "w_first": w_first.astype(jnp.bfloat16), "w_second": w_second.astype(jnp.bfloat16)}


def butterfly_stage(act_blocks, weights, distance):
    grouped = act_blocks.reshape(NUM_BLOCKS // (2 * distance), 2, distance, BLOCK_SIZE, act_blocks.shape[2])
    partner = grouped[:, ::-1].reshape(act_blocks.shape)
    paired = jnp.stack([act_blocks, partner], axis=1).astype(jnp.float32)
    mixed = jnp.einsum("ltij,ltjc->lic", weights.astype(jnp.float32), paired)
    return mixed.astype(jnp.bfloat16)


def apply_map(act_blocks, weights, distances):
    for stage, distance in enumerate(distances):
        act_blocks = butterfly_stage(act_blocks, weights[stage], distance)
    return act_blocks


def reference(signal, w_first, w_second):
    col_width = min(CHANNELS, 128)
    col_groups = CHANNELS // col_width
    grouped = signal.reshape(NUM_BLOCKS, BLOCK_SIZE, col_groups, col_width).transpose(2, 0, 1, 3)
    dist_down = [2 ** (STAGES - 1 - level) for level in range(STAGES)]
    dist_up = [2 ** level for level in range(STAGES)]

    def one_group(act_blocks):
        hidden = apply_map(act_blocks, w_first, dist_down)
        hidden = jax.nn.gelu(hidden.astype(jnp.float32), approximate=False).astype(jnp.bfloat16)
        return apply_map(hidden, w_second, dist_up)

    mapped = lax.map(one_group, grouped)
    return mapped.transpose(1, 2, 0, 3).reshape(SEQ_LEN, CHANNELS)
```

```python
import functools

import jax
import jax.numpy as jnp
from jax import lax
from jax.experimental import pallas as pl
from jax.experimental.pallas import tpu as pltpu
from jax.sharding import PartitionSpec as P

MESH = pl.DeviceIdType.MESH
BF = jnp.bfloat16
F32 = jnp.float32
LANES = 128


def spread(w):
    br = w.shape[0]
    fold = LANES // br
    lane = lax.broadcasted_iota(jnp.int32, w.shape, 1) // br
    zero = jnp.zeros_like(w)
    return jnp.concatenate([jnp.where(lane == k, w, zero) for k in range(fold)], axis=0)


def pair_tile(za, zb, wa, wb):
    top = jnp.concatenate([spread(wa[0]), spread(wa[1])], axis=1)
    low = jnp.concatenate([spread(wb[1]), spread(wb[0])], axis=1)
    lhs = jnp.concatenate([top, low], axis=0)
    rhs = jnp.concatenate([za, zb], axis=0)
    out = jnp.dot(lhs, rhs, preferred_element_type=F32)
    rows = za.shape[0]
    return out[:rows], out[rows:]


def own_tile(own, other, w):
    lhs = jnp.concatenate([spread(w[0]), spread(w[1])], axis=1)
    return jnp.dot(lhs, jnp.concatenate([own, other], axis=0), preferred_element_type=F32)


def swap_rows(z, dist, br):
    n = z.shape[0] // br
    return jnp.concatenate([z[(k ^ dist) * br:((k ^ dist) + 1) * br] for k in range(n)], axis=0)


def radix4(zs, ws, order):
    zs = list(zs)
    for stage, dist in enumerate(order):
        new = [None] * 4
        for a in range(4):
            b = a ^ dist
            if a < b:
                oa, ob = pair_tile(zs[a], zs[b], ws[stage][a], ws[stage][b])
                new[a], new[b] = oa.astype(BF), ob.astype(BF)
        zs = new
    return zs


def gelu(x):
    return 0.5 * x * (1.0 + lax.erf(x * 0.7071067811865476))


def kernel(chips, sig, w1t, w1l, w2l, w2t, out,
           t1, z2, zs1, zm, zs2, t2, wl, wt,
           a1s, a1r, p1s, p1r, a2s, a2r, p2s, p2r, d1s, d1r, d2s, d2r, a3s, a3r, a4s, a4r,
           lsem, wsem, osem):
    d = lax.axis_index("sp")
    x = d // 2
    c = d % 2
    sib = x * 2 + (1 - c)
    br = wl.shape[3]
    gr = LANES // br * br
    nk = z2.shape[0]
    no = z2.shape[2] // gr
    ch = z2.shape[2]

    def peer(r):
        return (x + r) % chips

    def dev(q):
        return {"sp": q * 2 + c}

    barrier = pltpu.get_barrier_semaphore()
    for r in range(1, chips):
        pl.semaphore_signal(barrier, inc=1, device_id=dev(peer(r)), device_id_type=MESH)
    pl.semaphore_signal(barrier, inc=1, device_id={"sp": sib}, device_id_type=MESH)

    def rows_of(q, k):
        return pl.ds(pl.multiple_of((q * nk + k) * ch, ch), ch)

    def load_w(i):
        src = w1l.at[i] if i < w1l.shape[0] else w2l.at[i - w1l.shape[0]]
        return pltpu.make_async_copy(src, wl.at[i], wsem.at[i])

    def own_a1(k):
        return pltpu.make_async_copy(sig.at[rows_of(x, k)], t1.at[k, x], lsem.at[k])

    def wt_rows(q, k):
        return pl.ds((q * nk + k) * no, no)

    def own_p1(k):
        return pltpu.make_async_copy(w1t.at[wt_rows(x, k)], wt.at[0, k, x], lsem.at[nk + k])

    def own_p2(k):
        return pltpu.make_async_copy(w2t.at[wt_rows(x, k)], wt.at[1, k, x], lsem.at[2 * nk + k])

    for k in range(nk):
        own_a1(k).start()
        own_p1(k).start()
    for i in range(wl.shape[0]):
        load_w(i).start()
    for k in range(nk):
        own_p2(k).start()
    pl.semaphore_wait(barrier, chips)

    def slot(k, r):
        return k * (chips - 1) + (r - 1)

    def remote(src, dst, ss, rs, i, q):
        return pltpu.make_async_remote_copy(src, dst, ss.at[i], rs.at[i], device_id=dev(q), device_id_type=MESH)

    def a1(k, r):
        return remote(sig.at[rows_of(peer(r), k)], t1.at[k, x], a1s, a1r, slot(k, r), peer(r))

    def p1(k, r):
        return remote(w1t.at[wt_rows(peer(r), k)], wt.at[0, k, x], p1s, p1r, slot(k, r), peer(r))

    def a2(k, r):
        return remote(t1.at[k, peer(r)], z2.at[k, x], a2s, a2r, slot(k, r), peer(r))

    def p2(k, r):
        return remote(w2t.at[wt_rows(peer(r), k)], wt.at[1, k, x], p2s, p2r, slot(k, r), peer(r))

    def a3(k, r):
        return remote(t1.at[k, peer(r)], t2.at[k, x], a3s, a3r, slot(k, r), peer(r))

    def a4(k, r):
        return remote(t2.at[k, peer(r)], out.at[rows_of(x, k)], a4s, a4r, slot(k, r), peer(r))

    def d1(k):
        return pltpu.make_async_remote_copy(z2.at[k], zs1.at[k], d1s.at[k], d1r.at[k], device_id={"sp": sib}, device_id_type=MESH)

    def d2(k):
        return pltpu.make_async_remote_copy(zm.at[k], zs2.at[k], d2s.at[k], d2r.at[k], device_id={"sp": sib}, device_id_type=MESH)

    def own_a2(k):
        return pltpu.make_async_copy(t1.at[k, x], z2.at[k, x], osem.at[k])

    def own_a3(k):
        return pltpu.make_async_copy(t1.at[k, x], t2.at[k, x], osem.at[nk + k])

    def own_a4(k):
        return pltpu.make_async_copy(t2.at[k, x], out.at[rows_of(x, k)], osem.at[2 * nk + k])

    for k in range(nk):
        for r in range(1, chips):
            p1(k, r).start()
            a1(k, r).start()

    def grp(o):
        return pl.ds(o * gr, gr)

    def gidx(k, q, o):
        return (q * nk + k) * no + o

    def t_stage(buf, m, k, order):
        for o in range(no):
            ws = [[(wt[m, k, p, o, s, 0], wt[m, k, p, o, s, 1]) for p in range(chips)] for s in range(2)]
            zs = radix4([buf[k, p, grp(o), :] for p in range(chips)], ws, order)
            for p in range(chips):
                buf[k, p, grp(o), :] = zs[p]

    @pl.loop(0, nk)
    def _(k):
        own_a1(k).wait()
        own_p1(k).wait()
        for r in range(1, chips):
            p1(k, r).wait_recv()
            a1(k, r).wait_recv()
        t_stage(t1, 0, k, (2, 1))
        own_a2(k).start()
        for r in range(1, chips):
            a2(k, r).start()

    for k in range(nk):
        for r in range(1, chips):
            p2(k, r).start()
    for i in range(wl.shape[0]):
        load_w(i).wait()

    def wpair(i, g):
        return wl[i, g, 0], wl[i, g, 1]

    @pl.loop(0, nk)
    def _(k):
        own_a2(k).wait()
        for r in range(1, chips):
            a2(k, r).wait_recv()
        d1(k).start()

    @pl.loop(0, nk)
    def _(k):
        d1(k).wait_recv()
        for o in range(no):
            zs = []
            for q in range(chips):
                g = gidx(k, q, o)
                zs.append(own_tile(z2[k, q, grp(o), :], zs1[k, q, grp(o), :], wpair(0, g)).astype(BF))
            ws = [[wpair(1 + s, gidx(k, q, o)) for q in range(chips)] for s in range(2)]
            zs = radix4(zs, ws, (2, 1))
            for q in range(chips):
                zm[k, q, grp(o), :] = zs[q]

    def pass_k(first, order):
        @pl.loop(0, chips)
        def _(q):
            for o in range(no):
                ws = [[wpair(first + s, gidx(k, q, o)) for k in range(nk)] for s in range(2)]
                zs = radix4([zm[k, q, grp(o), :] for k in range(nk)], ws, order)
                for k in range(nk):
                    zm[k, q, grp(o), :] = zs[k]

    def pass_o(first, order):
        @pl.loop(0, nk)
        def _(k):
            for q in range(chips):
                ws = [[wpair(first + s, gidx(k, q, o)) for o in range(no)] for s in range(2)]
                zs = radix4([zm[k, q, grp(o), :] for o in range(no)], ws, order)
                for o in range(no):
                    zm[k, q, grp(o), :] = zs[o]

    pass_k(3, (2, 1))
    pass_o(5, (2, 1))

    @pl.loop(0, nk)
    def _(k):
        @pl.loop(0, chips)
        def _(q):
            zs = [zm[k, q, grp(o), :] for o in range(no)]
            gs = [gidx(k, q, o) for o in range(no)]
            zs = [own_tile(z, swap_rows(z, 2, br), wpair(7, g)).astype(BF) for z, g in zip(zs, gs)]
            zs = [own_tile(z, swap_rows(z, 1, br), wpair(8, g)).astype(BF) for z, g in zip(zs, gs)]
            zs = [gelu(z.astype(F32)).astype(BF) for z in zs]
            zs = [own_tile(z, swap_rows(z, 1, br), wpair(9, g)).astype(BF) for z, g in zip(zs, gs)]
            zs = [own_tile(z, swap_rows(z, 2, br), wpair(10, g)).astype(BF) for z, g in zip(zs, gs)]
            for o in range(no):
                zm[k, q, grp(o), :] = zs[o]

    pass_o(11, (1, 2))
    pass_k(13, (1, 2))

    for k in range(nk):
        for r in range(1, chips):
            a1(k, r).wait_send()
            p1(k, r).wait_send()
            a2(k, r).wait_send()

    @pl.loop(0, nk)
    def _(k):
        for o in range(no):
            ws = [[wpair(15 + s, gidx(k, q, o)) for q in range(chips)] for s in range(2)]
            zs = radix4([zm[k, q, grp(o), :] for q in range(chips)], ws, (1, 2))
            for q in range(chips):
                zm[k, q, grp(o), :] = zs[q]
        d2(k).start()

    @pl.loop(0, nk)
    def _(k):
        d2(k).wait_recv()
        for o in range(no):
            for q in range(chips):
                z = own_tile(zm[k, q, grp(o), :], zs2[k, q, grp(o), :], wpair(17, gidx(k, q, o)))
                t1[k, q, grp(o), :] = z.astype(BF)
        own_a3(k).start()
        for r in range(1, chips):
            a3(k, r).start()

    @pl.loop(0, nk)
    def _(k):
        own_a3(k).wait()
        own_p2(k).wait()
        for r in range(1, chips):
            p2(k, r).wait_recv()
            a3(k, r).wait_recv()
        t_stage(t2, 1, k, (1, 2))
        own_a4(k).start()
        for r in range(1, chips):
            a4(k, r).start()

    @pl.loop(0, nk)
    def _(k):
        own_a4(k).wait()
        d1(k).wait_send()
        d2(k).wait_send()
        for r in range(1, chips):
            a4(k, r).wait_recv()
            p2(k, r).wait_send()
            a3(k, r).wait_send()
            a4(k, r).wait_send()


def solution(mesh):
    chips = mesh.shape["sp"] // 2

    def prep(w):
        st, nb, two, br, _ = w.shape
        fold = LANES // br
        w = w.reshape(st, nb // fold, fold, two, br, br)
        return w.transpose(0, 1, 3, 4, 2, 5).reshape(st, nb // fold, two, br, LANES)

    def device_program(signal, w_first, w_second):
        rows, cols = signal.shape
        st, nb, two, br, _ = w_first.shape
        fold = LANES // br
        nk = 4
        ch = rows // (chips * nk)
        no = ch // (fold * br)
        w1 = prep(w_first)
        w2 = prep(w_second)
        w1t, w1l = w1[:2].transpose(1, 0, 2, 3, 4), w1[2:]
        w2l, w2t = w2[:st - 2], w2[st - 2:].transpose(1, 0, 2, 3, 4)
        buf = pltpu.VMEM((nk, chips, ch, cols), BF)
        ns = nk * (chips - 1)
        pairs = [ns, ns, ns, ns, nk, nk, ns, ns]
        sems = [pltpu.SemaphoreType.DMA((n,)) for n in pairs for _ in range(2)]
        hbm = pl.BlockSpec(memory_space=pl.ANY)
        return pl.pallas_call(
            functools.partial(kernel, chips),
            out_shape=jax.ShapeDtypeStruct((rows, cols), BF),
            in_specs=[hbm] * 5,
            out_specs=hbm,
            scratch_shapes=[
                buf, buf, buf, buf, buf, buf,
                pltpu.VMEM((2 * (st - 2), nb // fold, two, br, LANES), BF),
                pltpu.VMEM((2, nk, chips, no, 2, two, br, LANES), BF),
                *sems,
                pltpu.SemaphoreType.DMA((3 * nk,)),
                pltpu.SemaphoreType.DMA((2 * (st - 2),)),
                pltpu.SemaphoreType.DMA((3 * nk,)),
            ],
            compiler_params=pltpu.CompilerParams(
                collective_id=0, has_side_effects=True, vmem_limit_bytes=60 * 2**20
            ),
        )(signal, w1t, w1l, w2l, w2t)

    row_spec = P(("dp", "sp"), None)
    weight_spec = P(None, "sp", None, None, None)
    return jax.shard_map(device_program, mesh=mesh, in_specs=(row_spec, weight_spec, weight_spec), out_specs=row_spec, check_vma=False)
```

```python
import functools

import jax
import jax.numpy as jnp
from jax import lax
from jax.experimental import pallas as pl
from jax.experimental.pallas import tpu as pltpu
from jax.sharding import PartitionSpec as P

MESH = pl.DeviceIdType.MESH
BF = jnp.bfloat16
F32 = jnp.float32
LANES = 128


def spread(w):
    br = w.shape[0]
    fold = LANES // br
    lane = lax.broadcasted_iota(jnp.int32, w.shape, 1) // br
    zero = jnp.zeros_like(w)
    return jnp.concatenate([jnp.where(lane == k, w, zero) for k in range(fold)], axis=0)


def pair_tile(za, zb, wa, wb):
    top = jnp.concatenate([spread(wa[0]), spread(wa[1])], axis=1)
    low = jnp.concatenate([spread(wb[1]), spread(wb[0])], axis=1)
    lhs = jnp.concatenate([top, low], axis=0)
    rhs = jnp.concatenate([za, zb], axis=0)
    out = jnp.dot(lhs, rhs, preferred_element_type=F32)
    rows = za.shape[0]
    return out[:rows], out[rows:]


def own_tile(own, other, w):
    lhs = jnp.concatenate([spread(w[0]), spread(w[1])], axis=1)
    return jnp.dot(lhs, jnp.concatenate([own, other], axis=0), preferred_element_type=F32)


def swap_rows(z, dist, br):
    n = z.shape[0] // br
    return jnp.concatenate([z[(k ^ dist) * br:((k ^ dist) + 1) * br] for k in range(n)], axis=0)


def radix4(zs, ws, order):
    zs = list(zs)
    for stage, dist in enumerate(order):
        new = [None] * 4
        for a in range(4):
            b = a ^ dist
            if a < b:
                oa, ob = pair_tile(zs[a], zs[b], ws[stage][a], ws[stage][b])
                new[a], new[b] = oa.astype(BF), ob.astype(BF)
        zs = new
    return zs


def gelu(x):
    return 0.5 * x * (1.0 + lax.erf(x * 0.7071067811865476))


def prep_stage(raw, mid, perm, sel, dst):
    two, br, _, nb = raw.shape
    fold = LANES // br
    lane = lax.broadcasted_iota(jnp.int32, (br, nb), 1) % fold
    zero = jnp.zeros((br, nb), BF)
    tile = perm.shape[0] // 16
    unroll = 8

    @pl.loop(0, br // unroll)
    def _(h):
        for u in range(unroll):
            i = h * unroll + u
            rhs = jnp.concatenate([jnp.where(lane == k, raw[t, i], zero) for t in range(two) for k in range(fold)], axis=0)
            y = lax.dot_general(sel[...], rhs, (((1,), (1,)), ((), ())), preferred_element_type=F32)
            mid[i] = y.astype(BF)

    @pl.loop(0, nb // fold // tile // 2)
    def _(h):
        for u in range(2):
            g0 = (h * 2 + u) * tile
            for half in range(br // 16):
                rhs = jnp.concatenate([mid[half * 16 + v, pl.ds(pl.multiple_of(g0, tile), tile), :] for v in range(16)], axis=0)
                res = jnp.dot(perm[...], rhs, preferred_element_type=F32).astype(BF)
                for g in range(tile):
                    for t in range(two):
                        dst[g0 + g, t, half * 16:(half + 1) * 16, :] = res[g * 16:(g + 1) * 16, t * LANES:(t + 1) * LANES]


def kernel(chips, sig, w1, w2, out,
           t1, z2, zs1, zm, zs2, t2, wl, wt, raw, mid, perm, sel,
           a1s, a1r, p1s, p1r, a2s, a2r, p2s, p2r, d1s, d1r, d2s, d2r, a3s, a3r, a4s, a4r,
           lsem, wsem, osem):
    d = lax.axis_index("sp")
    x = d // 2
    c = d % 2
    sib = x * 2 + (1 - c)
    br = wl.shape[3]
    gr = LANES // br * br
    nk = z2.shape[0]
    no = z2.shape[2] // gr
    ch = z2.shape[2]

    def peer(r):
        return (x + r) % chips

    def dev(q):
        return {"sp": q * 2 + c}

    barrier = pltpu.get_barrier_semaphore()
    for r in range(1, chips):
        pl.semaphore_signal(barrier, inc=1, device_id=dev(peer(r)), device_id_type=MESH)
    pl.semaphore_signal(barrier, inc=1, device_id={"sp": sib}, device_id_type=MESH)

    def rows_of(q, k):
        return pl.ds(pl.multiple_of((q * nk + k) * ch, ch), ch)

    st = w1.shape[0]

    two = wl.shape[2]
    last = 2 * st - 1

    def load_w(w, stage, n):
        return pltpu.make_async_copy(w.at[stage], raw.at[n % 2], wsem.at[n % 2])

    def load_job(n):
        @pl.when(n < st)
        def _():
            load_w(w1, n, n).start()

        @pl.when((n >= st) & (n <= last))
        def _():
            load_w(w2, (n - 2) % st, n).start()

    def jobs(lo, hi):
        @pl.loop(lo, hi)
        def _(n):
            load_job(n + 1)
            load_w(w1, 0, n).wait()
            prep_stage(raw.at[n % 2], mid, perm, sel, wl.at[n])

    def own_a1(k):
        return pltpu.make_async_copy(sig.at[rows_of(x, k)], t1.at[k, x], lsem.at[k])

    def wt_rows(q, k):
        return pl.ds((q * nk + k) * no, no)

    def own_p1(k):
        return pltpu.make_async_copy(wl.at[pl.ds(0, 2), wt_rows(x, k)], wt.at[0, k, x], lsem.at[nk + k])

    def own_p2(k):
        return pltpu.make_async_copy(wl.at[pl.ds(st, 2), wt_rows(x, k)], wt.at[1, k, x], lsem.at[2 * nk + k])

    load_w(w1, 0, 0).start()
    for k in range(nk):
        own_a1(k).start()
    row = lax.broadcasted_iota(jnp.int32, perm.shape, 0)
    col = lax.broadcasted_iota(jnp.int32, perm.shape, 1)
    tile = perm.shape[0] // 16
    perm[...] = (col == row % 16 * tile + row // 16).astype(F32).astype(BF)
    row = lax.broadcasted_iota(jnp.int32, sel.shape, 0)
    col = lax.broadcasted_iota(jnp.int32, sel.shape, 1)
    sel[...] = (row == col // (LANES // br)).astype(F32).astype(BF)
    pl.semaphore_wait(barrier, chips)

    def slot(k, r):
        return k * (chips - 1) + (r - 1)

    def remote(src, dst, ss, rs, i, q):
        return pltpu.make_async_remote_copy(src, dst, ss.at[i], rs.at[i], device_id=dev(q), device_id_type=MESH)

    def a1(k, r):
        return remote(sig.at[rows_of(peer(r), k)], t1.at[k, x], a1s, a1r, slot(k, r), peer(r))

    def p1(k, r):
        return remote(wl.at[pl.ds(0, 2), wt_rows(peer(r), k)], wt.at[0, k, x], p1s, p1r, slot(k, r), peer(r))

    def a2(k, r):
        return remote(t1.at[k, peer(r)], z2.at[k, x], a2s, a2r, slot(k, r), peer(r))

    def p2(k, r):
        return remote(wl.at[pl.ds(st, 2), wt_rows(peer(r), k)], wt.at[1, k, x], p2s, p2r, slot(k, r), peer(r))

    def a3(k, r):
        return remote(t1.at[k, peer(r)], t2.at[k, x], a3s, a3r, slot(k, r), peer(r))

    def a4(k, r):
        return remote(t2.at[k, peer(r)], out.at[rows_of(x, k)], a4s, a4r, slot(k, r), peer(r))

    def d1(k):
        return pltpu.make_async_remote_copy(z2.at[k], zs1.at[k], d1s.at[k], d1r.at[k], device_id={"sp": sib}, device_id_type=MESH)

    def d2(k):
        return pltpu.make_async_remote_copy(zm.at[k], zs2.at[k], d2s.at[k], d2r.at[k], device_id={"sp": sib}, device_id_type=MESH)

    def own_a2(k):
        return pltpu.make_async_copy(t1.at[k, x], z2.at[k, x], osem.at[k])

    def own_a3(k):
        return pltpu.make_async_copy(t1.at[k, x], t2.at[k, x], osem.at[nk + k])

    def own_a4(k):
        return pltpu.make_async_copy(t2.at[k, x], out.at[rows_of(x, k)], osem.at[2 * nk + k])

    def send_a1(k):
        for r in range(1, chips):
            a1(k, r).start()

    def send_p1(k):
        own_p1(k).start()
        for r in range(1, chips):
            p1(k, r).start()

    send_a1(0)
    send_a1(1)
    jobs(0, 2)
    send_p1(0)
    send_p1(1)
    for k in range(2, nk):
        send_a1(k)
        send_p1(k)

    def grp(o):
        return pl.ds(o * gr, gr)

    def gidx(k, q, o):
        return (q * nk + k) * no + o

    def t_stage(buf, m, k, order):
        for o in range(no):
            ws = [[(wt[m, k, p, s, o, 0], wt[m, k, p, s, o, 1]) for p in range(chips)] for s in range(2)]
            zs = radix4([buf[k, p, grp(o), :] for p in range(chips)], ws, order)
            for p in range(chips):
                buf[k, p, grp(o), :] = zs[p]

    @pl.loop(0, nk)
    def _(k):
        jobs(2 + 4 * k, 6 + 4 * k)
        own_a1(k).wait()
        own_p1(k).wait()
        for r in range(1, chips):
            p1(k, r).wait_recv()
            a1(k, r).wait_recv()
        t_stage(t1, 0, k, (2, 1))
        own_a2(k).start()
        for r in range(1, chips):
            a2(k, r).start()

    for k in range(nk):
        own_p2(k).start()
        for r in range(1, chips):
            p2(k, r).start()
    jobs(2 + 4 * nk, 2 * st)

    def wpair(i, g):
        return wl[i, g, 0], wl[i, g, 1]

    @pl.loop(0, nk)
    def _(k):
        own_a2(k).wait()
        for r in range(1, chips):
            a2(k, r).wait_recv()
        d1(k).start()

    @pl.loop(0, nk)
    def _(k):
        d1(k).wait_recv()
        for o in range(no):
            zs = []
            for q in range(chips):
                g = gidx(k, q, o)
                zs.append(own_tile(z2[k, q, grp(o), :], zs1[k, q, grp(o), :], wpair(2, g)).astype(BF))
            ws = [[wpair(3 + s, gidx(k, q, o)) for q in range(chips)] for s in range(2)]
            zs = radix4(zs, ws, (2, 1))
            for q in range(chips):
                zm[k, q, grp(o), :] = zs[q]

    def pass_k(first, order):
        @pl.loop(0, chips)
        def _(q):
            for o in range(no):
                ws = [[wpair(first + s, gidx(k, q, o)) for k in range(nk)] for s in range(2)]
                zs = radix4([zm[k, q, grp(o), :] for k in range(nk)], ws, order)
                for k in range(nk):
                    zm[k, q, grp(o), :] = zs[k]

    def pass_o(first, order):
        @pl.loop(0, nk)
        def _(k):
            for q in range(chips):
                ws = [[wpair(first + s, gidx(k, q, o)) for o in range(no)] for s in range(2)]
                zs = radix4([zm[k, q, grp(o), :] for o in range(no)], ws, order)
                for o in range(no):
                    zm[k, q, grp(o), :] = zs[o]

    pass_k(5, (2, 1))
    pass_o(7, (2, 1))

    @pl.loop(0, nk)
    def _(k):
        @pl.loop(0, chips)
        def _(q):
            zs = [zm[k, q, grp(o), :] for o in range(no)]
            gs = [gidx(k, q, o) for o in range(no)]
            zs = [own_tile(z, swap_rows(z, 2, br), wpair(9, g)).astype(BF) for z, g in zip(zs, gs)]
            zs = [own_tile(z, swap_rows(z, 1, br), wpair(10, g)).astype(BF) for z, g in zip(zs, gs)]
            zs = [gelu(z.astype(F32)).astype(BF) for z in zs]
            zs = [own_tile(z, swap_rows(z, 1, br), wpair(st + 2, g)).astype(BF) for z, g in zip(zs, gs)]
            zs = [own_tile(z, swap_rows(z, 2, br), wpair(st + 3, g)).astype(BF) for z, g in zip(zs, gs)]
            for o in range(no):
                zm[k, q, grp(o), :] = zs[o]

    pass_o(st + 4, (1, 2))
    pass_k(st + 6, (1, 2))

    for k in range(nk):
        for r in range(1, chips):
            a1(k, r).wait_send()
            p1(k, r).wait_send()
            a2(k, r).wait_send()

    @pl.loop(0, nk)
    def _(k):
        for o in range(no):
            ws = [[wpair(st + 8 + s, gidx(k, q, o)) for q in range(chips)] for s in range(2)]
            zs = radix4([zm[k, q, grp(o), :] for q in range(chips)], ws, (1, 2))
            for q in range(chips):
                zm[k, q, grp(o), :] = zs[q]
        d2(k).start()

    @pl.loop(0, nk)
    def _(k):
        d2(k).wait_recv()
        for o in range(no):
            for q in range(chips):
                z = own_tile(zm[k, q, grp(o), :], zs2[k, q, grp(o), :], wpair(st + 10, gidx(k, q, o)))
                t1[k, q, grp(o), :] = z.astype(BF)
        own_a3(k).start()
        for r in range(1, chips):
            a3(k, r).start()

    @pl.loop(0, nk)
    def _(k):
        own_a3(k).wait()
        own_p2(k).wait()
        for r in range(1, chips):
            p2(k, r).wait_recv()
            a3(k, r).wait_recv()
        t_stage(t2, 1, k, (1, 2))
        own_a4(k).start()
        for r in range(1, chips):
            a4(k, r).start()

    @pl.loop(0, nk)
    def _(k):
        own_a4(k).wait()
        d1(k).wait_send()
        d2(k).wait_send()
        for r in range(1, chips):
            a4(k, r).wait_recv()
            p2(k, r).wait_send()
            a3(k, r).wait_send()
            a4(k, r).wait_send()


def solution(mesh):
    chips = mesh.shape["sp"] // 2

    def device_program(signal, w_first, w_second):
        rows, cols = signal.shape
        st, nb, two, br, _ = w_first.shape
        fold = LANES // br
        nk = 4
        ch = rows // (chips * nk)
        no = ch // (fold * br)
        w1 = w_first.transpose(0, 2, 3, 4, 1)
        w2 = w_second.transpose(0, 2, 3, 4, 1)
        buf = pltpu.VMEM((nk, chips, ch, cols), BF)
        ns = nk * (chips - 1)
        pairs = [ns, ns, ns, ns, nk, nk, ns, ns]
        sems = [pltpu.SemaphoreType.DMA((n,)) for n in pairs for _ in range(2)]
        hbm = pl.BlockSpec(memory_space=pl.ANY)
        return pl.pallas_call(
            functools.partial(kernel, chips),
            out_shape=jax.ShapeDtypeStruct((rows, cols), BF),
            in_specs=[hbm] * 3,
            out_specs=hbm,
            scratch_shapes=[
                buf, buf, buf, buf, buf, buf,
                pltpu.VMEM((2 * st, nb // fold, two, br, LANES), BF),
                pltpu.VMEM((2, nk, chips, 2, no, two, br, LANES), BF),
                pltpu.VMEM((2, two, br, br, nb), BF),
                pltpu.VMEM((br, nb // fold, two * LANES), BF),
                pltpu.VMEM((nb, nb), BF),
                pltpu.VMEM((nb // fold, nb), BF),
                *sems,
                pltpu.SemaphoreType.DMA((3 * nk,)),
                pltpu.SemaphoreType.DMA((2,)),
                pltpu.SemaphoreType.DMA((3 * nk,)),
            ],
            compiler_params=pltpu.CompilerParams(
                collective_id=0, has_side_effects=True, vmem_limit_bytes=60 * 2**20
            ),
        )(signal, w1, w2)

    row_spec = P(("dp", "sp"), None)
    weight_spec = P(None, "sp", None, None, None)
    return jax.shard_map(device_program, mesh=mesh, in_specs=(row_spec, weight_spec, weight_spec), out_specs=row_spec, check_vma=False)
```

```python
import functools

import jax
import jax.numpy as jnp
from jax import lax
from jax.experimental import pallas as pl
from jax.experimental.pallas import tpu as pltpu
from jax.sharding import PartitionSpec as P

MESH = pl.DeviceIdType.MESH
BF = jnp.bfloat16
F32 = jnp.float32
LANES = 128


def lane_masks(shape, br):
    lane = lax.broadcasted_iota(jnp.int32, shape, 1)
    return [(lane >= k * br) & (lane < (k + 1) * br) for k in range(LANES // br)]


def spread(w, masks):
    zero = jnp.zeros_like(w)
    return jnp.concatenate([jnp.where(m, w, zero) for m in masks], axis=0)


def pair_tile(masks, za, zb, wa, wb):
    top = jnp.concatenate([spread(wa[0], masks), spread(wa[1], masks)], axis=1)
    low = jnp.concatenate([spread(wb[1], masks), spread(wb[0], masks)], axis=1)
    lhs = jnp.concatenate([top, low], axis=0)
    rhs = jnp.concatenate([za, zb], axis=0)
    out = jnp.dot(lhs, rhs, preferred_element_type=F32)
    rows = za.shape[0]
    return out[:rows], out[rows:]


def own_tile(masks, own, other, w):
    lhs = jnp.concatenate([spread(w[0], masks), spread(w[1], masks)], axis=1)
    return jnp.dot(lhs, jnp.concatenate([own, other], axis=0), preferred_element_type=F32)


def swap_rows(z, dist, br):
    n = z.shape[0] // br
    return jnp.concatenate([z[(k ^ dist) * br:((k ^ dist) + 1) * br] for k in range(n)], axis=0)


def radix4(masks, zs, ws, order):
    zs = list(zs)
    for stage, dist in enumerate(order):
        new = [None] * 4
        for a in range(4):
            b = a ^ dist
            if a < b:
                oa, ob = pair_tile(masks, zs[a], zs[b], ws[stage][a], ws[stage][b])
                new[a], new[b] = oa.astype(BF), ob.astype(BF)
        zs = new
    return zs


def gelu(x):
    return 0.5 * x * (1.0 + lax.erf(x * 0.7071067811865476))


def prep_stage(nk, raw, mid, perm, sel, dst):
    two, br, _, nb = raw.shape
    fold = LANES // br
    lane = lax.broadcasted_iota(jnp.int32, (br, nb), 1) // nk % fold
    zero = jnp.zeros((br, nb), BF)
    tile = perm.shape[0] // 16
    unroll = 8

    @pl.loop(0, br // unroll)
    def _(h):
        for u in range(unroll):
            i = h * unroll + u
            rhs = jnp.concatenate([jnp.where(lane == k, raw[t, i], zero) for t in range(two) for k in range(fold)], axis=0)
            y = lax.dot_general(sel[...], rhs, (((1,), (1,)), ((), ())), preferred_element_type=F32)
            mid[i] = y.astype(BF)

    @pl.loop(0, nb // fold // tile // 2)
    def _(h):
        for u in range(2):
            g0 = (h * 2 + u) * tile
            for half in range(br // 16):
                rhs = jnp.concatenate([mid[half * 16 + v, pl.ds(pl.multiple_of(g0, tile), tile), :] for v in range(16)], axis=0)
                res = jnp.dot(perm[...], rhs, preferred_element_type=F32).astype(BF)
                for g in range(tile):
                    for t in range(two):
                        dst[g0 + g, t, half * 16:(half + 1) * 16, :] = res[g * 16:(g + 1) * 16, t * LANES:(t + 1) * LANES]


def kernel(chips, sig, w1, w2, out,
           t1, z2, zs1, zm, zs2, t2, wl, wt, raw, mid, perm, sel,
           a1s, a1r, p1s, p1r, a2s, a2r, p2s, p2r, d1s, d1r, d2s, d2r, a3s, a3r, a4s, a4r,
           lsem, wsem, osem):
    d = lax.axis_index("sp")
    x = d // 2
    c = d % 2
    sib = x * 2 + (1 - c)
    br = wl.shape[3]
    fold = LANES // br
    nk = z2.shape[0]
    no = z2.shape[2] // fold

    def peer(r):
        return (x + r) % chips

    def dev(q):
        return {"sp": q * 2 + c}

    barrier = pltpu.get_barrier_semaphore()
    for r in range(1, chips):
        pl.semaphore_signal(barrier, inc=1, device_id=dev(peer(r)), device_id_type=MESH)
    pl.semaphore_signal(barrier, inc=1, device_id={"sp": sib}, device_id_type=MESH)

    st = w1.shape[0]

    two = wl.shape[2]
    last = 2 * st - 1

    def load_w(w, stage, n):
        return pltpu.make_async_copy(w.at[stage], raw.at[n % 2], wsem.at[n % 2])

    def load_job(n):
        @pl.when(n < st)
        def _():
            load_w(w1, n, n).start()

        @pl.when((n >= st) & (n <= last))
        def _():
            load_w(w2, (n - 2) % st, n).start()

    def jobs(lo, hi):
        @pl.loop(lo, hi)
        def _(n):
            load_job(n + 1)
            load_w(w1, 0, n).wait()
            prep_stage(nk, raw.at[n % 2], mid, perm, sel, wl.at[n])

    def own_a1(k):
        return pltpu.make_async_copy(sig.at[x, :, k], t1.at[k, x], lsem.at[k])

    def wt_rows(q, k):
        return pl.ds((q * nk + k) * no, no)

    def own_p1(k):
        return pltpu.make_async_copy(wl.at[pl.ds(0, 2), wt_rows(x, k)], wt.at[0, k, x], lsem.at[nk + k])

    def own_p2(k):
        return pltpu.make_async_copy(wl.at[pl.ds(st, 2), wt_rows(x, k)], wt.at[1, k, x], lsem.at[2 * nk + k])

    load_w(w1, 0, 0).start()
    for k in range(nk):
        own_a1(k).start()
    row = lax.broadcasted_iota(jnp.int32, perm.shape, 0)
    col = lax.broadcasted_iota(jnp.int32, perm.shape, 1)
    tile = perm.shape[0] // 16
    perm[...] = (col == row % 16 * tile + row // 16).astype(F32).astype(BF)
    row = lax.broadcasted_iota(jnp.int32, sel.shape, 0)
    col = lax.broadcasted_iota(jnp.int32, sel.shape, 1)
    span = no * fold * nk
    sel[...] = (row == (col // span * nk + col % nk) * no + col // (fold * nk) % no).astype(F32).astype(BF)
    pl.semaphore_wait(barrier, chips)

    def slot(k, r):
        return k * (chips - 1) + (r - 1)

    def remote(src, dst, ss, rs, i, q):
        return pltpu.make_async_remote_copy(src, dst, ss.at[i], rs.at[i], device_id=dev(q), device_id_type=MESH)

    def a1(k, r):
        return remote(sig.at[peer(r), :, k], t1.at[k, x], a1s, a1r, slot(k, r), peer(r))

    def p1(k, r):
        return remote(wl.at[pl.ds(0, 2), wt_rows(peer(r), k)], wt.at[0, k, x], p1s, p1r, slot(k, r), peer(r))

    def a2(k, r):
        return remote(t1.at[k, peer(r)], z2.at[k, x], a2s, a2r, slot(k, r), peer(r))

    def p2(k, r):
        return remote(wl.at[pl.ds(st, 2), wt_rows(peer(r), k)], wt.at[1, k, x], p2s, p2r, slot(k, r), peer(r))

    def a3(k, r):
        return remote(t1.at[k, peer(r)], t2.at[k, x], a3s, a3r, slot(k, r), peer(r))

    def a4(k, r):
        return remote(t2.at[k, peer(r)], out.at[x, :, k], a4s, a4r, slot(k, r), peer(r))

    def d1(k):
        return pltpu.make_async_remote_copy(z2.at[k], zs1.at[k], d1s.at[k], d1r.at[k], device_id={"sp": sib}, device_id_type=MESH)

    def d2(k):
        return pltpu.make_async_remote_copy(zm.at[k], zs2.at[k], d2s.at[k], d2r.at[k], device_id={"sp": sib}, device_id_type=MESH)

    def own_a2(k):
        return pltpu.make_async_copy(t1.at[k, x], z2.at[k, x], osem.at[k])

    def own_a3(k):
        return pltpu.make_async_copy(t1.at[k, x], t2.at[k, x], osem.at[nk + k])

    def own_a4(k):
        return pltpu.make_async_copy(t2.at[k, x], out.at[x, :, k], osem.at[2 * nk + k])

    def send_a1(k):
        for r in range(1, chips):
            a1(k, r).start()

    def send_p1(k):
        own_p1(k).start()
        for r in range(1, chips):
            p1(k, r).start()

    send_a1(0)
    send_a1(1)
    jobs(0, 2)
    send_p1(0)
    send_p1(1)
    for k in range(2, nk):
        send_a1(k)
        send_p1(k)

    def get(buf, k, q, o):
        return buf[k, q, o * fold:(o + 1) * fold].reshape(fold * br, buf.shape[4])

    def put(buf, k, q, o, z):
        buf[k, q, o * fold:(o + 1) * fold] = z.reshape(fold, br, buf.shape[4])

    masks = lane_masks((br, LANES), br)

    def gidx(k, q, o):
        return (q * nk + k) * no + o

    def t_stage(buf, m, k, order):
        for o in range(no):
            ws = [[(wt[m, k, p, s, o, 0], wt[m, k, p, s, o, 1]) for p in range(chips)] for s in range(2)]
            zs = radix4(masks, [get(buf, k, p, o) for p in range(chips)], ws, order)
            for p in range(chips):
                put(buf, k, p, o, zs[p])

    @pl.loop(0, nk)
    def _(k):
        jobs(2 + 4 * k, 6 + 4 * k)
        own_a1(k).wait()
        own_p1(k).wait()
        for r in range(1, chips):
            p1(k, r).wait_recv()
            a1(k, r).wait_recv()
        t_stage(t1, 0, k, (2, 1))
        own_a2(k).start()
        for r in range(1, chips):
            a2(k, r).start()

    jobs(2 + 4 * nk, 2 * st)

    def wpair(i, g):
        return wl[i, g, 0], wl[i, g, 1]

    def within(zs, gs, i, dist):
        return [own_tile(masks, z, swap_rows(z, dist, br), wpair(i, g)).astype(BF) for z, g in zip(zs, gs)]

    def over_q(k, o, zs, first, order):
        ws = [[wpair(first + s, gidx(k, q, o)) for q in range(chips)] for s in range(2)]
        return radix4(masks, zs, ws, order)

    def over_o(k, q, zs, first, order):
        ws = [[wpair(first + s, gidx(k, q, o)) for o in range(no)] for s in range(2)]
        return radix4(masks, zs, ws, order)

    def far_local(k):
        d1(k).wait_recv()
        for o in range(no):
            zs = [own_tile(masks, get(z2, k, q, o), get(zs1, k, q, o), wpair(2, gidx(k, q, o))).astype(BF) for q in range(chips)]
            for q, z in enumerate(over_q(k, o, zs, 3, (2, 1))):
                put(zm, k, q, o, z)
        for q in range(chips):
            gs = [gidx(k, q, o) for o in range(no)]
            zs = over_o(k, q, [get(zm, k, q, o) for o in range(no)], 5, (2, 1))
            zs = within(within(zs, gs, 7, 2), gs, 8, 1)
            for o in range(no):
                put(zm, k, q, o, zs[o])

    def near_local(k):
        for q in range(chips):
            gs = [gidx(k, q, o) for o in range(no)]
            zs = within(within([get(zm, k, q, o) for o in range(no)], gs, st + 4, 1), gs, st + 5, 2)
            for o, z in enumerate(over_o(k, q, zs, st + 6, (1, 2))):
                put(zm, k, q, o, z)
        for o in range(no):
            for q, z in enumerate(over_q(k, o, [get(zm, k, q, o) for q in range(chips)], st + 8, (1, 2))):
                put(zm, k, q, o, z)

    @pl.loop(0, nk + 1)
    def _(k):
        @pl.when(k < nk)
        def _():
            own_a2(k).wait()
            for r in range(1, chips):
                a2(k, r).wait_recv()
            d1(k).start()

        @pl.when(k == nk)
        def _():
            for j in range(nk):
                own_p2(j).start()
                for r in range(1, chips):
                    p2(j, r).start()

        @pl.when(k > 0)
        def _():
            far_local(k - 1)

    @pl.loop(0, chips)
    def _(q):
        for o in range(no):
            zs = [get(zm, k, q, o) for k in range(nk)]
            gs = [gidx(k, q, o) for k in range(nk)]
            zs = radix4(masks, zs, [[wpair(9 + s, g) for g in gs] for s in range(2)], (2, 1))
            zs = [gelu(z.astype(F32)).astype(BF) for z in zs]
            zs = radix4(masks, zs, [[wpair(st + 2 + s, g) for g in gs] for s in range(2)], (1, 2))
            for k in range(nk):
                put(zm, k, q, o, zs[k])

    for k in range(nk):
        for r in range(1, chips):
            a1(k, r).wait_send()
            p1(k, r).wait_send()
            a2(k, r).wait_send()

    @pl.loop(0, nk + 1)
    def _(k):
        @pl.when(k < nk)
        def _():
            near_local(k)
            d2(k).start()

        @pl.when(k > 0)
        def _():
            j = k - 1
            d2(j).wait_recv()
            for o in range(no):
                for q in range(chips):
                    put(t1, j, q, o, own_tile(masks, get(zm, j, q, o), get(zs2, j, q, o), wpair(st + 10, gidx(j, q, o))).astype(BF))
            own_a3(j).start()
            for r in range(1, chips):
                a3(j, r).start()

    @pl.loop(0, nk)
    def _(k):
        own_a3(k).wait()
        own_p2(k).wait()
        for r in range(1, chips):
            p2(k, r).wait_recv()
            a3(k, r).wait_recv()
        t_stage(t2, 1, k, (1, 2))
        own_a4(k).start()
        for r in range(1, chips):
            a4(k, r).start()

    @pl.loop(0, nk)
    def _(k):
        own_a4(k).wait()
        d1(k).wait_send()
        d2(k).wait_send()
        for r in range(1, chips):
            a4(k, r).wait_recv()
            p2(k, r).wait_send()
            a3(k, r).wait_send()
            a4(k, r).wait_send()


def solution(mesh):
    chips = mesh.shape["sp"] // 2

    def device_program(signal, w_first, w_second):
        rows, cols = signal.shape
        st, nb, two, br, _ = w_first.shape
        fold = LANES // br
        nk = 4
        no = nb // (chips * nk * fold)
        signal = signal.reshape(chips, no * fold, nk, br, cols)
        w1 = w_first.transpose(0, 2, 3, 4, 1)
        w2 = w_second.transpose(0, 2, 3, 4, 1)
        buf = pltpu.VMEM((nk, chips, no * fold, br, cols), BF)
        ns = nk * (chips - 1)
        pairs = [ns, ns, ns, ns, nk, nk, ns, ns]
        sems = [pltpu.SemaphoreType.DMA((n,)) for n in pairs for _ in range(2)]
        hbm = pl.BlockSpec(memory_space=pl.ANY)
        res = pl.pallas_call(
            functools.partial(kernel, chips),
            out_shape=jax.ShapeDtypeStruct(signal.shape, BF),
            in_specs=[hbm] * 3,
            out_specs=hbm,
            scratch_shapes=[
                buf, buf, buf, buf, buf, buf,
                pltpu.VMEM((2 * st, nb // fold, two, br, LANES), BF),
                pltpu.VMEM((2, nk, chips, 2, no, two, br, LANES), BF),
                pltpu.VMEM((2, two, br, br, nb), BF),
                pltpu.VMEM((br, nb // fold, two * LANES), BF),
                pltpu.VMEM((nb, nb), BF),
                pltpu.VMEM((nb // fold, nb), BF),
                *sems,
                pltpu.SemaphoreType.DMA((3 * nk,)),
                pltpu.SemaphoreType.DMA((2,)),
                pltpu.SemaphoreType.DMA((3 * nk,)),
            ],
            compiler_params=pltpu.CompilerParams(
                collective_id=0, has_side_effects=True, vmem_limit_bytes=60 * 2**20
            ),
        )(signal, w1, w2)
        return res.reshape(rows, cols)

    row_spec = P(("dp", "sp"), None)
    weight_spec = P(None, "sp", None, None, None)
    return jax.shard_map(device_program, mesh=mesh, in_specs=(row_spec, weight_spec, weight_spec), out_specs=row_spec, check_vma=False)
```

```python
import functools

import jax
import jax.numpy as jnp
from jax import lax
from jax.experimental import pallas as pl
from jax.experimental.pallas import tpu as pltpu
from jax.sharding import PartitionSpec as P

MESH = pl.DeviceIdType.MESH
BF = jnp.bfloat16
F32 = jnp.float32
LANES = 128


def lane_masks(shape, br):
    lane = lax.broadcasted_iota(jnp.int32, shape, 1)
    return [(lane >= k * br) & (lane < (k + 1) * br) for k in range(LANES // br)]


def spread(w, masks):
    zero = jnp.zeros_like(w)
    return jnp.concatenate([jnp.where(m, w, zero) for m in masks], axis=0)


def pair_tile(masks, za, zb, wa, wb):
    top = jnp.concatenate([spread(wa[0], masks), spread(wa[1], masks)], axis=1)
    low = jnp.concatenate([spread(wb[1], masks), spread(wb[0], masks)], axis=1)
    lhs = jnp.concatenate([top, low], axis=0)
    rhs = jnp.concatenate([za, zb], axis=0)
    out = jnp.dot(lhs, rhs, preferred_element_type=F32)
    rows = za.shape[0]
    return out[:rows], out[rows:]


def own_tile(masks, own, other, w):
    lhs = jnp.concatenate([spread(w[0], masks), spread(w[1], masks)], axis=1)
    return jnp.dot(lhs, jnp.concatenate([own, other], axis=0), preferred_element_type=F32)


def swap_rows(z, dist, br):
    n = z.shape[0] // br
    return jnp.concatenate([z[(k ^ dist) * br:((k ^ dist) + 1) * br] for k in range(n)], axis=0)


def radix4(masks, zs, ws, order):
    zs = list(zs)
    for stage, dist in enumerate(order):
        new = [None] * 4
        for a in range(4):
            b = a ^ dist
            if a < b:
                oa, ob = pair_tile(masks, zs[a], zs[b], ws[stage][a], ws[stage][b])
                new[a], new[b] = oa.astype(BF), ob.astype(BF)
        zs = new
    return zs


def gelu(x):
    return 0.5 * x * (1.0 + lax.erf(x * 0.7071067811865476))


def prep_stage(nk, raw, mid, perm, sel, dst):
    two, br, _, nb = raw.shape
    fold = LANES // br
    lane = lax.broadcasted_iota(jnp.int32, (br, nb), 1) // nk % fold
    zero = jnp.zeros((br, nb), BF)
    tile = perm.shape[0] // 16
    unroll = 8

    @pl.loop(0, br // unroll)
    def _(h):
        for u in range(unroll):
            i = h * unroll + u
            rhs = jnp.concatenate([jnp.where(lane == k, raw[t, i], zero) for t in range(two) for k in range(fold)], axis=0)
            y = lax.dot_general(sel[...], rhs, (((1,), (1,)), ((), ())), preferred_element_type=F32)
            mid[i] = y.astype(BF)

    @pl.loop(0, nb // fold // tile // 2)
    def _(h):
        for u in range(2):
            g0 = (h * 2 + u) * tile
            for half in range(br // 16):
                rhs = jnp.concatenate([mid[half * 16 + v, pl.ds(pl.multiple_of(g0, tile), tile), :] for v in range(16)], axis=0)
                res = jnp.dot(perm[...], rhs, preferred_element_type=F32).astype(BF)
                for g in range(tile):
                    for t in range(two):
                        dst[g0 + g, t, half * 16:(half + 1) * 16, :] = res[g * 16:(g + 1) * 16, t * LANES:(t + 1) * LANES]


def kernel(chips, sig, w1, w2, out,
           t1, z2, zs1, zm, zs2, t2, wl, wt, raw, mid, perm, sel,
           a1s, a1r, p1s, p1r, a2s, a2r, p2s, p2r, d1s, d1r, d2s, d2r, a3s, a3r, a4s, a4r, f1s, f1r, f2s, f2r,
           lsem, wsem, osem):
    d = lax.axis_index("sp")
    x = d // 2
    c = d % 2
    sib = x * 2 + (1 - c)
    group = lax.axis_index("dp")
    side = group % 2
    mate = group + 1 - 2 * side
    br = wl.shape[3]
    fold = LANES // br
    nk = z2.shape[0]
    no = z2.shape[2] // fold

    def peer(r):
        return (x + r) % chips

    def dev(q):
        return {"sp": q * 2 + c}

    barrier = pltpu.get_barrier_semaphore()
    for r in range(1, chips):
        pl.semaphore_signal(barrier, inc=1, device_id=dev(peer(r)), device_id_type=MESH)
    pl.semaphore_signal(barrier, inc=1, device_id={"sp": sib}, device_id_type=MESH)
    pl.semaphore_signal(barrier, inc=1, device_id={"dp": mate}, device_id_type=MESH)

    st = w1.shape[0]

    two = wl.shape[2]
    last = 2 * st - 1

    def load_w(w, stage, n):
        return pltpu.make_async_copy(w.at[stage], raw.at[n % 2], wsem.at[n % 2])

    def load_job(n):
        @pl.when(n < st)
        def _():
            load_w(w1, n, n).start()

        @pl.when((n >= st) & (n <= last))
        def _():
            load_w(w2, (n - 2) % st, n).start()

    def jobs(lo, hi):
        @pl.loop(lo, hi)
        def _(n):
            load_job(n + 1)
            load_w(w1, 0, n).wait()
            prep_stage(nk, raw.at[n % 2], mid, perm, sel, wl.at[n])

    def own_a1(k):
        return pltpu.make_async_copy(sig.at[x, :, k], t1.at[k, x], lsem.at[k])

    def wt_rows(q, k):
        return pl.ds((q * nk + k) * no, no)

    def own_p1(k):
        return pltpu.make_async_copy(wl.at[pl.ds(0, 2), wt_rows(x, k)], wt.at[0, k, x], lsem.at[nk + k])

    def own_p2(k):
        return pltpu.make_async_copy(wl.at[pl.ds(st, 2), wt_rows(x, k)], wt.at[1, k, x], lsem.at[2 * nk + k])

    load_w(w1, 0, 0).start()
    for k in range(nk):
        own_a1(k).start()
    row = lax.broadcasted_iota(jnp.int32, perm.shape, 0)
    col = lax.broadcasted_iota(jnp.int32, perm.shape, 1)
    tile = perm.shape[0] // 16
    perm[...] = (col == row % 16 * tile + row // 16).astype(F32).astype(BF)
    row = lax.broadcasted_iota(jnp.int32, sel.shape, 0)
    col = lax.broadcasted_iota(jnp.int32, sel.shape, 1)
    span = no * fold * nk
    sel[...] = (row == (col // span * nk + col % nk) * no + col // (fold * nk) % no).astype(F32).astype(BF)
    pl.semaphore_wait(barrier, chips + 1)

    def slot(k, r):
        return k * (chips - 1) + (r - 1)

    def remote(src, dst, ss, rs, i, q):
        return pltpu.make_async_remote_copy(src, dst, ss.at[i], rs.at[i], device_id=dev(q), device_id_type=MESH)

    def a1(k, r):
        return remote(sig.at[peer(r), :, k], t1.at[k, x], a1s, a1r, slot(k, r), peer(r))

    def cross(m, i, r):
        k = 2 * i + side
        return remote(wl.at[pl.ds(m * st, 2), wt_rows(peer(r), k)], wt.at[m, k, x], (p1s, p2s)[m], (p1r, p2r)[m], slot(i, r), peer(r))

    def share(m, i, r):
        k = 2 * i + side
        ref = wt.at[m, k, peer(r)]
        return pltpu.make_async_remote_copy(
            ref, ref, (f1s, f2s)[m].at[slot(i, r)], (f1r, f2r)[m].at[slot(i, r)], device_id={"dp": mate}, device_id_type=MESH)

    def forward(m, i):
        for r in range(1, chips):
            cross(m, i, r).wait_recv()
        for r in range(1, chips):
            share(m, i, r).start()

    def wait_shared(m, k):
        @pl.when(k % 2 != side)
        def _():
            for r in range(1, chips):
                share(m, k // 2, r).wait_recv()

    def a2(k, r):
        return remote(t1.at[k, peer(r)], z2.at[k, x], a2s, a2r, slot(k, r), peer(r))

    def a3(k, r):
        return remote(t1.at[k, peer(r)], t2.at[k, x], a3s, a3r, slot(k, r), peer(r))

    def a4(k, r):
        return remote(t2.at[k, peer(r)], out.at[x, :, k], a4s, a4r, slot(k, r), peer(r))

    def d1(k):
        return pltpu.make_async_remote_copy(z2.at[k], zs1.at[k], d1s.at[k], d1r.at[k], device_id={"sp": sib}, device_id_type=MESH)

    def d2(k):
        return pltpu.make_async_remote_copy(zm.at[k], zs2.at[k], d2s.at[k], d2r.at[k], device_id={"sp": sib}, device_id_type=MESH)

    def own_a2(k):
        return pltpu.make_async_copy(t1.at[k, x], z2.at[k, x], osem.at[k])

    def own_a3(k):
        return pltpu.make_async_copy(t1.at[k, x], t2.at[k, x], osem.at[nk + k])

    def own_a4(k):
        return pltpu.make_async_copy(t2.at[k, x], out.at[x, :, k], osem.at[2 * nk + k])

    def send_a1(k):
        for r in range(1, chips):
            a1(k, r).start()

    send_a1(0)
    send_a1(1)
    jobs(0, 2)
    for i in range(nk // 2):
        for r in range(1, chips):
            cross(0, i, r).start()
    for k in range(2, nk):
        send_a1(k)
    for k in range(nk):
        own_p1(k).start()

    def get(buf, k, q, o):
        return buf[k, q, o * fold:(o + 1) * fold].reshape(fold * br, buf.shape[4])

    def put(buf, k, q, o, z):
        buf[k, q, o * fold:(o + 1) * fold] = z.reshape(fold, br, buf.shape[4])

    masks = lane_masks((br, LANES), br)

    def gidx(k, q, o):
        return (q * nk + k) * no + o

    def t_stage(buf, m, k, order):
        for o in range(no):
            ws = [[(wt[m, k, p, s, o, 0], wt[m, k, p, s, o, 1]) for p in range(chips)] for s in range(2)]
            zs = radix4(masks, [get(buf, k, p, o) for p in range(chips)], ws, order)
            for p in range(chips):
                put(buf, k, p, o, zs[p])

    @pl.loop(0, nk // 2)
    def _(i):
        jobs(2 + 6 * i, 8 + 3 * i)
        forward(0, i)

    @pl.loop(0, nk)
    def _(k):
        jobs(11 + 2 * k, 13 + 2 * k)
        own_a1(k).wait()
        own_p1(k).wait()
        wait_shared(0, k)
        for r in range(1, chips):
            a1(k, r).wait_recv()
        t_stage(t1, 0, k, (2, 1))
        own_a2(k).start()
        for r in range(1, chips):
            a2(k, r).start()

    jobs(11 + 2 * nk, 2 * st)

    def wpair(i, g):
        return wl[i, g, 0], wl[i, g, 1]

    def within(zs, gs, i, dist):
        return [own_tile(masks, z, swap_rows(z, dist, br), wpair(i, g)).astype(BF) for z, g in zip(zs, gs)]

    def over_q(k, o, zs, first, order):
        ws = [[wpair(first + s, gidx(k, q, o)) for q in range(chips)] for s in range(2)]
        return radix4(masks, zs, ws, order)

    def over_o(k, q, zs, first, order):
        ws = [[wpair(first + s, gidx(k, q, o)) for o in range(no)] for s in range(2)]
        return radix4(masks, zs, ws, order)

    def far_local(k):
        d1(k).wait_recv()
        for o in range(no):
            zs = [own_tile(masks, get(z2, k, q, o), get(zs1, k, q, o), wpair(2, gidx(k, q, o))).astype(BF) for q in range(chips)]
            for q, z in enumerate(over_q(k, o, zs, 3, (2, 1))):
                put(zm, k, q, o, z)
        for q in range(chips):
            gs = [gidx(k, q, o) for o in range(no)]
            zs = over_o(k, q, [get(zm, k, q, o) for o in range(no)], 5, (2, 1))
            zs = within(within(zs, gs, 7, 2), gs, 8, 1)
            for o in range(no):
                put(zm, k, q, o, zs[o])

    def near_local(k):
        for q in range(chips):
            gs = [gidx(k, q, o) for o in range(no)]
            zs = within(within([get(zm, k, q, o) for o in range(no)], gs, st + 4, 1), gs, st + 5, 2)
            for o, z in enumerate(over_o(k, q, zs, st + 6, (1, 2))):
                put(zm, k, q, o, z)
        for o in range(no):
            for q, z in enumerate(over_q(k, o, [get(zm, k, q, o) for q in range(chips)], st + 8, (1, 2))):
                put(zm, k, q, o, z)

    @pl.loop(0, nk + 1)
    def _(k):
        @pl.when(k < nk)
        def _():
            own_a2(k).wait()
            for r in range(1, chips):
                a2(k, r).wait_recv()
            d1(k).start()

        @pl.when(k == nk)
        def _():
            for i in range(nk // 2):
                for r in range(1, chips):
                    cross(1, i, r).start()
            for j in range(nk):
                own_p2(j).start()

        @pl.when(k > 0)
        def _():
            far_local(k - 1)

    @pl.loop(0, chips)
    def _(q):
        for o in range(no):
            zs = [get(zm, k, q, o) for k in range(nk)]
            gs = [gidx(k, q, o) for k in range(nk)]
            zs = radix4(masks, zs, [[wpair(9 + s, g) for g in gs] for s in range(2)], (2, 1))
            zs = [gelu(z.astype(F32)).astype(BF) for z in zs]
            zs = radix4(masks, zs, [[wpair(st + 2 + s, g) for g in gs] for s in range(2)], (1, 2))
            for k in range(nk):
                put(zm, k, q, o, zs[k])

    @pl.loop(0, nk // 2)
    def _(i):
        forward(1, i)

    for k in range(nk):
        for r in range(1, chips):
            a1(k, r).wait_send()
            a2(k, r).wait_send()

    @pl.loop(0, nk + 1)
    def _(k):
        @pl.when(k < nk)
        def _():
            near_local(k)
            d2(k).start()

        @pl.when(k > 0)
        def _():
            j = k - 1
            d2(j).wait_recv()
            for o in range(no):
                for q in range(chips):
                    put(t1, j, q, o, own_tile(masks, get(zm, j, q, o), get(zs2, j, q, o), wpair(st + 10, gidx(j, q, o))).astype(BF))
            own_a3(j).start()
            for r in range(1, chips):
                a3(j, r).start()

    @pl.loop(0, nk)
    def _(k):
        own_a3(k).wait()
        own_p2(k).wait()
        wait_shared(1, k)
        for r in range(1, chips):
            a3(k, r).wait_recv()
        t_stage(t2, 1, k, (1, 2))
        own_a4(k).start()
        for r in range(1, chips):
            a4(k, r).start()

    @pl.loop(0, nk)
    def _(k):
        own_a4(k).wait()
        d1(k).wait_send()
        d2(k).wait_send()
        for r in range(1, chips):
            a4(k, r).wait_recv()
            a3(k, r).wait_send()
            a4(k, r).wait_send()

    @pl.loop(0, nk // 2)
    def _(i):
        for m in range(2):
            for r in range(1, chips):
                cross(m, i, r).wait_send()
                share(m, i, r).wait_send()


def solution(mesh):
    chips = mesh.shape["sp"] // 2

    def device_program(signal, w_first, w_second):
        rows, cols = signal.shape
        st, nb, two, br, _ = w_first.shape
        fold = LANES // br
        nk = 4
        no = nb // (chips * nk * fold)
        signal = signal.reshape(chips, no * fold, nk, br, cols)
        w1 = w_first.transpose(0, 2, 3, 4, 1)
        w2 = w_second.transpose(0, 2, 3, 4, 1)
        buf = pltpu.VMEM((nk, chips, no * fold, br, cols), BF)
        ns = nk * (chips - 1)
        pairs = [ns, ns // 2, ns, ns // 2, nk, nk, ns, ns, ns // 2, ns // 2]
        sems = [pltpu.SemaphoreType.DMA((n,)) for n in pairs for _ in range(2)]
        hbm = pl.BlockSpec(memory_space=pl.ANY)
        res = pl.pallas_call(
            functools.partial(kernel, chips),
            out_shape=jax.ShapeDtypeStruct(signal.shape, BF),
            in_specs=[hbm] * 3,
            out_specs=hbm,
            scratch_shapes=[
                buf, buf, buf, buf, buf, buf,
                pltpu.VMEM((2 * st, nb // fold, two, br, LANES), BF),
                pltpu.VMEM((2, nk, chips, 2, no, two, br, LANES), BF),
                pltpu.VMEM((2, two, br, br, nb), BF),
                pltpu.VMEM((br, nb // fold, two * LANES), BF),
                pltpu.VMEM((nb, nb), BF),
                pltpu.VMEM((nb // fold, nb), BF),
                *sems,
                pltpu.SemaphoreType.DMA((3 * nk,)),
                pltpu.SemaphoreType.DMA((2,)),
                pltpu.SemaphoreType.DMA((3 * nk,)),
            ],
            compiler_params=pltpu.CompilerParams(
                collective_id=0, has_side_effects=True, vmem_limit_bytes=60 * 2**20
            ),
        )(signal, w1, w2)
        return res.reshape(rows, cols)

    row_spec = P(("dp", "sp"), None)
    weight_spec = P(None, "sp", None, None, None)
    return jax.shard_map(device_program, mesh=mesh, in_specs=(row_spec, weight_spec, weight_spec), out_specs=row_spec, check_vma=False)
```

```python
import functools

import jax
import jax.numpy as jnp
from jax import lax
from jax.experimental import pallas as pl
from jax.experimental.pallas import tpu as pltpu
from jax.sharding import PartitionSpec as P

MESH = pl.DeviceIdType.MESH
BF = jnp.bfloat16
F32 = jnp.float32
LANES = 128


def lane_masks(shape, br):
    lane = lax.broadcasted_iota(jnp.int32, shape, 1)
    return [(lane >= k * br) & (lane < (k + 1) * br) for k in range(LANES // br)]


def spread(w, masks):
    zero = jnp.zeros_like(w)
    return jnp.concatenate([jnp.where(m, w, zero) for m in masks], axis=0)


def pair_tile(masks, za, zb, wa, wb):
    top = jnp.concatenate([spread(wa[0], masks), spread(wa[1], masks)], axis=1)
    low = jnp.concatenate([spread(wb[1], masks), spread(wb[0], masks)], axis=1)
    lhs = jnp.concatenate([top, low], axis=0)
    rhs = jnp.concatenate([za, zb], axis=0)
    out = jnp.dot(lhs, rhs, preferred_element_type=F32)
    rows = za.shape[0]
    return out[:rows], out[rows:]


def own_tile(masks, own, other, w):
    lhs = jnp.concatenate([spread(w[0], masks), spread(w[1], masks)], axis=1)
    return jnp.dot(lhs, jnp.concatenate([own, other], axis=0), preferred_element_type=F32)


def swap_rows(z, dist, br):
    n = z.shape[0] // br
    return jnp.concatenate([z[(k ^ dist) * br:((k ^ dist) + 1) * br] for k in range(n)], axis=0)


def gelu(x):
    return 0.5 * x * (1.0 + lax.erf(x * 0.7071067811865476))


def prep_stage(nk, raw, mid, perm, sel, dst):
    two, br, _, nb = raw.shape
    fold = LANES // br
    lane = lax.broadcasted_iota(jnp.int32, (br, nb), 1) // nk % fold
    zero = jnp.zeros((br, nb), BF)
    tile = perm.shape[0] // 16
    unroll = 8

    @pl.loop(0, br // unroll)
    def _(h):
        for u in range(unroll):
            i = h * unroll + u
            rhs = jnp.concatenate([jnp.where(lane == k, raw[t, i], zero) for t in range(two) for k in range(fold)], axis=0)
            y = lax.dot_general(sel[...], rhs, (((1,), (1,)), ((), ())), preferred_element_type=F32)
            mid[i] = y.astype(BF)

    @pl.loop(0, nb // fold // tile // 2)
    def _(h):
        for u in range(2):
            g0 = (h * 2 + u) * tile
            for half in range(br // 16):
                rhs = jnp.concatenate([mid[half * 16 + v, pl.ds(pl.multiple_of(g0, tile), tile), :] for v in range(16)], axis=0)
                res = jnp.dot(perm[...], rhs, preferred_element_type=F32).astype(BF)
                for g in range(tile):
                    for t in range(two):
                        dst[g0 + g, t, half * 16:(half + 1) * 16, :] = res[g * 16:(g + 1) * 16, t * LANES:(t + 1) * LANES]


def kernel(chips, sig, w1, w2, out,
           t1, z2, zs1, zm, zs2, t2, wl, wt, raw, mid, perm, sel,
           a1s, a1r, p1s, p1r, a2s, a2r, p2s, p2r, d1s, d1r, d2s, d2r, a3s, a3r, a4s, a4r, f1s, f1r, f2s, f2r,
           lsem, wsem, osem):
    d = lax.axis_index("sp")
    x = d // 2
    c = d % 2
    sib = x * 2 + (1 - c)
    group = lax.axis_index("dp")
    side = group % 2
    mate = group + 1 - 2 * side
    br = wl.shape[3]
    fold = LANES // br
    nk = z2.shape[0]
    no = z2.shape[2] // fold

    def peer(r):
        return (x + r) % chips

    def dev(q):
        return {"sp": q * 2 + c}

    barrier = pltpu.get_barrier_semaphore()
    for r in range(1, chips):
        pl.semaphore_signal(barrier, inc=1, device_id=dev(peer(r)), device_id_type=MESH)
    pl.semaphore_signal(barrier, inc=1, device_id={"sp": sib}, device_id_type=MESH)
    pl.semaphore_signal(barrier, inc=1, device_id={"dp": mate}, device_id_type=MESH)

    st = w1.shape[0]

    two = wl.shape[2]
    last = 2 * st - 1

    def load_w(w, stage, n):
        return pltpu.make_async_copy(w.at[stage], raw.at[n % 2], wsem.at[n % 2])

    def load_job(n):
        @pl.when(n < st)
        def _():
            load_w(w1, n, n).start()

        @pl.when((n >= st) & (n <= last))
        def _():
            load_w(w2, (n - 2) % st, n).start()

    def jobs(lo, hi):
        @pl.loop(lo, hi)
        def _(n):
            load_job(n + 1)
            load_w(w1, 0, n).wait()
            prep_stage(nk, raw.at[n % 2], mid, perm, sel, wl.at[n])

    def own_a1(k):
        return pltpu.make_async_copy(sig.at[x, :, k], t1.at[k, x], lsem.at[k])

    def wt_rows(q, k):
        return pl.ds((q * nk + k) * no, no)

    def own_p1(k):
        return pltpu.make_async_copy(wl.at[pl.ds(0, 2), wt_rows(x, k)], wt.at[0, k, x], lsem.at[nk + k])

    def own_p2(k):
        return pltpu.make_async_copy(wl.at[pl.ds(st, 2), wt_rows(x, k)], wt.at[1, k, x], lsem.at[2 * nk + k])

    load_w(w1, 0, 0).start()
    for k in range(nk):
        own_a1(k).start()
    row = lax.broadcasted_iota(jnp.int32, perm.shape, 0)
    col = lax.broadcasted_iota(jnp.int32, perm.shape, 1)
    tile = perm.shape[0] // 16
    perm[...] = (col == row % 16 * tile + row // 16).astype(F32).astype(BF)
    row = lax.broadcasted_iota(jnp.int32, sel.shape, 0)
    col = lax.broadcasted_iota(jnp.int32, sel.shape, 1)
    span = no * fold * nk
    sel[...] = (row == (col // span * nk + col % nk) * no + col // (fold * nk) % no).astype(F32).astype(BF)
    pl.semaphore_wait(barrier, chips + 1)

    def slot(k, r):
        return k * (chips - 1) + (r - 1)

    def remote(src, dst, ss, rs, i, q):
        return pltpu.make_async_remote_copy(src, dst, ss.at[i], rs.at[i], device_id=dev(q), device_id_type=MESH)

    def a1(k, r):
        return remote(sig.at[peer(r), :, k], t1.at[k, x], a1s, a1r, slot(k, r), peer(r))

    def cross(m, i, r):
        k = 2 * i + side
        return remote(wl.at[pl.ds(m * st, 2), wt_rows(peer(r), k)], wt.at[m, k, x], (p1s, p2s)[m], (p1r, p2r)[m], slot(i, r), peer(r))

    def share(m, i, r):
        k = 2 * i + side
        ref = wt.at[m, k, peer(r)]
        return pltpu.make_async_remote_copy(
            ref, ref, (f1s, f2s)[m].at[slot(i, r)], (f1r, f2r)[m].at[slot(i, r)], device_id={"dp": mate}, device_id_type=MESH)

    def forward(m, i):
        for r in range(1, chips):
            cross(m, i, r).wait_recv()
        for r in range(1, chips):
            share(m, i, r).start()

    def wait_shared(m, k):
        @pl.when(k % 2 != side)
        def _():
            for r in range(1, chips):
                share(m, k // 2, r).wait_recv()

    def a2(k, r):
        return remote(t1.at[k, peer(r)], z2.at[k, x], a2s, a2r, slot(k, r), peer(r))

    def a3(k, r):
        return remote(t1.at[k, peer(r)], t2.at[k, x], a3s, a3r, slot(k, r), peer(r))

    def a4(k, r):
        return remote(t2.at[k, peer(r)], out.at[x, :, k], a4s, a4r, slot(k, r), peer(r))

    def d1(k):
        return pltpu.make_async_remote_copy(z2.at[k], zs1.at[k], d1s.at[k], d1r.at[k], device_id={"sp": sib}, device_id_type=MESH)

    def d2(k):
        return pltpu.make_async_remote_copy(zm.at[k], zs2.at[k], d2s.at[k], d2r.at[k], device_id={"sp": sib}, device_id_type=MESH)

    def own_a2(k):
        return pltpu.make_async_copy(t1.at[k, x], z2.at[k, x], osem.at[k])

    def own_a3(k):
        return pltpu.make_async_copy(t1.at[k, x], t2.at[k, x], osem.at[nk + k])

    def own_a4(k):
        return pltpu.make_async_copy(t2.at[k, x], out.at[x, :, k], osem.at[2 * nk + k])

    def send_a1(k):
        for r in range(1, chips):
            a1(k, r).start()

    send_a1(0)
    send_a1(1)
    jobs(0, 2)
    for i in range(nk // 2):
        for r in range(1, chips):
            cross(0, i, r).start()
    for k in range(2, nk):
        send_a1(k)
    for k in range(nk):
        own_p1(k).start()

    def get(buf, k, q, o):
        return buf[k, q, o * fold:(o + 1) * fold].reshape(fold * br, buf.shape[4])

    def put(buf, k, q, o, z):
        buf[k, q, o * fold:(o + 1) * fold] = z.reshape(fold, br, buf.shape[4])

    masks = lane_masks((br, LANES), br)

    def gidx(k, q, o):
        return (q * nk + k) * no + o

    def pair_layer(buf, lines, dist, weight, post=None):
        for line in lines:
            for a in range(len(line)):
                b = a ^ dist
                if a < b:
                    ka, kb = line[a], line[b]
                    za, zb = pair_tile(masks, get(buf, *ka), get(buf, *kb), weight(*ka), weight(*kb))
                    if post is not None:
                        za, zb = post(za), post(zb)
                    put(buf, *ka, za.astype(BF))
                    put(buf, *kb, zb.astype(BF))

    def t_stage(buf, m, k, order):
        lines = [[(k, p, o) for p in range(chips)] for o in range(no)]
        for s, dist in enumerate(order):
            pair_layer(buf, lines, dist, lambda k, p, o: (wt[m, k, p, s, o, 0], wt[m, k, p, s, o, 1]))

    @pl.loop(0, nk // 2)
    def _(i):
        jobs(2 + 6 * i, 8 + 3 * i)
        forward(0, i)

    @pl.loop(0, nk)
    def _(k):
        jobs(11 + 2 * k, 13 + 2 * k)
        own_a1(k).wait()
        own_p1(k).wait()
        wait_shared(0, k)
        for r in range(1, chips):
            a1(k, r).wait_recv()
        t_stage(t1, 0, k, (2, 1))
        own_a2(k).start()
        for r in range(1, chips):
            a2(k, r).start()

    jobs(11 + 2 * nk, 2 * st)

    def wpair(i, g):
        return wl[i, g, 0], wl[i, g, 1]

    def local(i):
        return lambda k, q, o: wpair(i, gidx(k, q, o))

    def within(places, i, dist):
        for key in places:
            z = get(zm, *key)
            put(zm, *key, own_tile(masks, z, swap_rows(z, dist, br), local(i)(*key)).astype(BF))

    def over_q(k):
        return [[(k, q, o) for q in range(chips)] for o in range(no)]

    def over_o(k):
        return [[(k, q, o) for o in range(no)] for q in range(chips)]

    def places(k):
        return [(k, q, o) for q in range(chips) for o in range(no)]

    def far_local(k):
        d1(k).wait_recv()
        for key in places(k):
            put(zm, *key, own_tile(masks, get(z2, *key), get(zs1, *key), local(2)(*key)).astype(BF))
        pair_layer(zm, over_q(k), 2, local(3))
        pair_layer(zm, over_q(k), 1, local(4))
        pair_layer(zm, over_o(k), 2, local(5))
        pair_layer(zm, over_o(k), 1, local(6))
        within(places(k), 7, 2)
        within(places(k), 8, 1)

    def near_local(k):
        within(places(k), st + 4, 1)
        within(places(k), st + 5, 2)
        pair_layer(zm, over_o(k), 1, local(st + 6))
        pair_layer(zm, over_o(k), 2, local(st + 7))
        pair_layer(zm, over_q(k), 1, local(st + 8))
        pair_layer(zm, over_q(k), 2, local(st + 9))

    @pl.loop(0, nk + 1)
    def _(k):
        @pl.when(k < nk)
        def _():
            own_a2(k).wait()
            for r in range(1, chips):
                a2(k, r).wait_recv()
            d1(k).start()

        @pl.when(k == nk)
        def _():
            for i in range(nk // 2):
                for r in range(1, chips):
                    cross(1, i, r).start()
            for j in range(nk):
                own_p2(j).start()

        @pl.when(k > 0)
        def _():
            far_local(k - 1)

    @pl.loop(0, chips)
    def _(q):
        lines = [[(k, q, o) for k in range(nk)] for o in range(no)]
        pair_layer(zm, lines, 2, local(9))
        pair_layer(zm, lines, 1, local(10), lambda z: gelu(z.astype(BF).astype(F32)))
        pair_layer(zm, lines, 1, local(st + 2))
        pair_layer(zm, lines, 2, local(st + 3))

    @pl.loop(0, nk // 2)
    def _(i):
        forward(1, i)

    for k in range(nk):
        for r in range(1, chips):
            a1(k, r).wait_send()
            a2(k, r).wait_send()

    @pl.loop(0, nk + 1)
    def _(k):
        @pl.when(k < nk)
        def _():
            near_local(k)
            d2(k).start()

        @pl.when(k > 0)
        def _():
            j = k - 1
            d2(j).wait_recv()
            for o in range(no):
                for q in range(chips):
                    put(t1, j, q, o, own_tile(masks, get(zm, j, q, o), get(zs2, j, q, o), wpair(st + 10, gidx(j, q, o))).astype(BF))
            own_a3(j).start()
            for r in range(1, chips):
                a3(j, r).start()

    @pl.loop(0, nk)
    def _(k):
        own_a3(k).wait()
        own_p2(k).wait()
        wait_shared(1, k)
        for r in range(1, chips):
            a3(k, r).wait_recv()
        t_stage(t2, 1, k, (1, 2))
        own_a4(k).start()
        for r in range(1, chips):
            a4(k, r).start()

    @pl.loop(0, nk)
    def _(k):
        own_a4(k).wait()
        d1(k).wait_send()
        d2(k).wait_send()
        for r in range(1, chips):
            a4(k, r).wait_recv()
            a3(k, r).wait_send()
            a4(k, r).wait_send()

    @pl.loop(0, nk // 2)
    def _(i):
        for m in range(2):
            for r in range(1, chips):
                cross(m, i, r).wait_send()
                share(m, i, r).wait_send()


def solution(mesh):
    chips = mesh.shape["sp"] // 2

    def device_program(signal, w_first, w_second):
        rows, cols = signal.shape
        st, nb, two, br, _ = w_first.shape
        fold = LANES // br
        nk = 4
        no = nb // (chips * nk * fold)
        signal = signal.reshape(chips, no * fold, nk, br, cols)
        w1 = w_first.transpose(0, 2, 3, 4, 1)
        w2 = w_second.transpose(0, 2, 3, 4, 1)
        buf = pltpu.VMEM((nk, chips, no * fold, br, cols), BF)
        ns = nk * (chips - 1)
        pairs = [ns, ns // 2, ns, ns // 2, nk, nk, ns, ns, ns // 2, ns // 2]
        sems = [pltpu.SemaphoreType.DMA((n,)) for n in pairs for _ in range(2)]
        hbm = pl.BlockSpec(memory_space=pl.ANY)
        res = pl.pallas_call(
            functools.partial(kernel, chips),
            out_shape=pltpu.VMEM(signal.shape, BF),
            in_specs=[hbm] * 3,
            out_specs=pl.BlockSpec(memory_space=pltpu.VMEM),
            scratch_shapes=[
                buf, buf, buf, buf, buf, buf,
                pltpu.VMEM((2 * st, nb // fold, two, br, LANES), BF),
                pltpu.VMEM((2, nk, chips, 2, no, two, br, LANES), BF),
                pltpu.VMEM((2, two, br, br, nb), BF),
                pltpu.VMEM((br, nb // fold, two * LANES), BF),
                pltpu.VMEM((nb, nb), BF),
                pltpu.VMEM((nb // fold, nb), BF),
                *sems,
                pltpu.SemaphoreType.DMA((3 * nk,)),
                pltpu.SemaphoreType.DMA((2,)),
                pltpu.SemaphoreType.DMA((3 * nk,)),
            ],
            compiler_params=pltpu.CompilerParams(
                collective_id=0, has_side_effects=True, vmem_limit_bytes=56 * 2**20
            ),
        )(signal, w1, w2)
        return res.reshape(rows, cols)

    row_spec = P(("dp", "sp"), None)
    weight_spec = P(None, "sp", None, None, None)
    return jax.shard_map(device_program, mesh=mesh, in_specs=(row_spec, weight_spec, weight_spec), out_specs=row_spec, check_vma=False)
```

```python
import functools

import jax
import jax.numpy as jnp
from jax import lax
from jax.experimental import pallas as pl
from jax.experimental.pallas import tpu as pltpu
from jax.sharding import PartitionSpec as P

MESH = pl.DeviceIdType.MESH
BF = jnp.bfloat16
F32 = jnp.float32
LANES = 128


def lane_masks(shape, br):
    lane = lax.broadcasted_iota(jnp.int32, shape, 1)
    return [(lane >= k * br) & (lane < (k + 1) * br) for k in range(LANES // br)]


def spread(w, masks):
    zero = jnp.zeros_like(w)
    return jnp.concatenate([jnp.where(m, w, zero) for m in masks], axis=0)


def pair_tile(masks, za, zb, wa, wb):
    top = jnp.concatenate([spread(wa[0], masks), spread(wa[1], masks)], axis=1)
    low = jnp.concatenate([spread(wb[1], masks), spread(wb[0], masks)], axis=1)
    lhs = jnp.concatenate([top, low], axis=0)
    rhs = jnp.concatenate([za, zb], axis=0)
    out = jnp.dot(lhs, rhs, preferred_element_type=F32)
    rows = za.shape[0]
    return out[:rows], out[rows:]


def own_tile(masks, own, other, w):
    lhs = jnp.concatenate([spread(w[0], masks), spread(w[1], masks)], axis=1)
    return jnp.dot(lhs, jnp.concatenate([own, other], axis=0), preferred_element_type=F32)


def swap_rows(z, dist, br):
    n = z.shape[0] // br
    return jnp.concatenate([z[(k ^ dist) * br:((k ^ dist) + 1) * br] for k in range(n)], axis=0)


def gelu(x):
    return 0.5 * x * (1.0 + lax.erf(x * 0.7071067811865476))


def prep_stage(nk, raw, mid, perm, sel, dst):
    two, br, _, nb = raw.shape
    fold = LANES // br
    lane = lax.broadcasted_iota(jnp.int32, (br, nb), 1) // nk % fold
    zero = jnp.zeros((br, nb), BF)
    tile = perm.shape[0] // 16
    unroll = 8

    @pl.loop(0, br // unroll)
    def _(h):
        for u in range(unroll):
            i = h * unroll + u
            rhs = jnp.concatenate([jnp.where(lane == k, raw[t, i], zero) for t in range(two) for k in range(fold)], axis=0)
            y = lax.dot_general(sel[...], rhs, (((1,), (1,)), ((), ())), preferred_element_type=F32)
            mid[i] = y.astype(BF)

    @pl.loop(0, nb // fold // tile // 2)
    def _(h):
        for u in range(2):
            g0 = (h * 2 + u) * tile
            for half in range(br // 16):
                rhs = jnp.concatenate([mid[half * 16 + v, pl.ds(pl.multiple_of(g0, tile), tile), :] for v in range(16)], axis=0)
                res = jnp.dot(perm[...], rhs, preferred_element_type=F32).astype(BF)
                for g in range(tile):
                    for t in range(two):
                        dst[g0 + g, t, half * 16:(half + 1) * 16, :] = res[g * 16:(g + 1) * 16, t * LANES:(t + 1) * LANES]


def kernel(chips, ways, sig, w1, w2, out,
           t1, z2, zs1, zm, zs2, t2, wl, wt, raw, mid, perm, sel,
           a1s, a1r, p1s, p1r, a2s, a2r, p2s, p2r, d1s, d1r, d2s, d2r, a3s, a3r, a4s, a4r, f1s, f1r, f2s, f2r,
           lsem, wsem, osem):
    d = lax.axis_index("sp")
    x = d // 2
    c = d % 2
    sib = x * 2 + (1 - c)
    group = lax.axis_index("dp")
    side = group % ways

    def mate(j):
        return {"dp": group - side + (side + j) % ways}

    br = wl.shape[3]
    fold = LANES // br
    nk = z2.shape[0]
    no = z2.shape[2] // fold

    def peer(r):
        return (x + r) % chips

    def dev(q):
        return {"sp": q * 2 + c}

    barrier = pltpu.get_barrier_semaphore()
    for r in range(1, chips):
        pl.semaphore_signal(barrier, inc=1, device_id=dev(peer(r)), device_id_type=MESH)
    pl.semaphore_signal(barrier, inc=1, device_id={"sp": sib}, device_id_type=MESH)
    for j in range(1, ways):
        pl.semaphore_signal(barrier, inc=1, device_id=mate(j), device_id_type=MESH)

    st = w1.shape[0]

    two = wl.shape[2]
    last = 2 * st - 1

    def load_w(w, stage, n):
        return pltpu.make_async_copy(w.at[stage], raw.at[n % 2], wsem.at[n % 2])

    def load_job(n):
        @pl.when(n < st)
        def _():
            load_w(w1, n, n).start()

        @pl.when((n >= st) & (n <= last))
        def _():
            load_w(w2, (n - 2) % st, n).start()

    def jobs(lo, hi):
        @pl.loop(lo, hi)
        def _(n):
            load_job(n + 1)
            load_w(w1, 0, n).wait()
            prep_stage(nk, raw.at[n % 2], mid, perm, sel, wl.at[n])

    def own_a1(k):
        return pltpu.make_async_copy(sig.at[x, :, k], t1.at[k, x], lsem.at[k])

    def wt_rows(q, k):
        return pl.ds((q * nk + k) * no, no)

    def own_p1(k):
        return pltpu.make_async_copy(wl.at[pl.ds(0, 2), wt_rows(x, k)], wt.at[0, k, x], lsem.at[nk + k])

    def own_p2(k):
        return pltpu.make_async_copy(wl.at[pl.ds(st, 2), wt_rows(x, k)], wt.at[1, k, x], lsem.at[2 * nk + k])

    load_w(w1, 0, 0).start()
    for k in range(nk):
        own_a1(k).start()
    row = lax.broadcasted_iota(jnp.int32, perm.shape, 0)
    col = lax.broadcasted_iota(jnp.int32, perm.shape, 1)
    tile = perm.shape[0] // 16
    perm[...] = (col == row % 16 * tile + row // 16).astype(F32).astype(BF)
    row = lax.broadcasted_iota(jnp.int32, sel.shape, 0)
    col = lax.broadcasted_iota(jnp.int32, sel.shape, 1)
    span = no * fold * nk
    sel[...] = (row == (col // span * nk + col % nk) * no + col // (fold * nk) % no).astype(F32).astype(BF)
    pl.semaphore_wait(barrier, chips + ways - 1)

    def slot(k, r):
        return k * (chips - 1) + (r - 1)

    def remote(src, dst, ss, rs, i, q):
        return pltpu.make_async_remote_copy(src, dst, ss.at[i], rs.at[i], device_id=dev(q), device_id_type=MESH)

    def a1(k, r):
        return remote(sig.at[peer(r), :, k], t1.at[k, x], a1s, a1r, slot(k, r), peer(r))

    def cross(m, r):
        return remote(wl.at[pl.ds(m * st, 2), wt_rows(peer(r), side)], wt.at[m, side, x], (p1s, p2s)[m], (p1r, p2r)[m], r - 1, peer(r))

    def share(m, j, r):
        ref = wt.at[m, side, peer(r)]
        i = (j - 1) * (chips - 1) + r - 1
        return pltpu.make_async_remote_copy(
            ref, ref, (f1s, f2s)[m].at[i], (f1r, f2r)[m].at[i], device_id=mate(j), device_id_type=MESH)

    def forward(m):
        for r in range(1, chips):
            cross(m, r).wait_recv()
        for j in range(1, ways):
            for r in range(1, chips):
                share(m, j, r).start()

    def wait_shared(m, k):
        @pl.when(k != side)
        def _():
            for r in range(1, chips):
                share(m, (side - k + ways) % ways, r).wait_recv()

    def a2(k, r):
        return remote(t1.at[k, peer(r)], z2.at[k, x], a2s, a2r, slot(k, r), peer(r))

    def a3(k, r):
        return remote(t1.at[k, peer(r)], t2.at[k, x], a3s, a3r, slot(k, r), peer(r))

    def a4(k, r):
        return remote(t2.at[k, peer(r)], out.at[x, :, k], a4s, a4r, slot(k, r), peer(r))

    def d1(k):
        return pltpu.make_async_remote_copy(z2.at[k], zs1.at[k], d1s.at[k], d1r.at[k], device_id={"sp": sib}, device_id_type=MESH)

    def d2(k):
        return pltpu.make_async_remote_copy(zm.at[k], zs2.at[k], d2s.at[k], d2r.at[k], device_id={"sp": sib}, device_id_type=MESH)

    def own_a2(k):
        return pltpu.make_async_copy(t1.at[k, x], z2.at[k, x], osem.at[k])

    def own_a3(k):
        return pltpu.make_async_copy(t1.at[k, x], t2.at[k, x], osem.at[nk + k])

    def own_a4(k):
        return pltpu.make_async_copy(t2.at[k, x], out.at[x, :, k], osem.at[2 * nk + k])

    def send_a1(k):
        for r in range(1, chips):
            a1(k, r).start()

    send_a1(0)
    jobs(0, 2)
    for r in range(1, chips):
        cross(0, r).start()
    for k in range(1, nk):
        send_a1(k)
    for k in range(nk):
        own_p1(k).start()

    def get(buf, k, q, o):
        return buf[k, q, o * fold:(o + 1) * fold].reshape(fold * br, buf.shape[4])

    def put(buf, k, q, o, z):
        buf[k, q, o * fold:(o + 1) * fold] = z.reshape(fold, br, buf.shape[4])

    masks = lane_masks((br, LANES), br)

    def gidx(k, q, o):
        return (q * nk + k) * no + o

    def pair_layer(buf, lines, dist, weight, post=None):
        for line in lines:
            for a in range(len(line)):
                b = a ^ dist
                if a < b:
                    ka, kb = line[a], line[b]
                    za, zb = pair_tile(masks, get(buf, *ka), get(buf, *kb), weight(*ka), weight(*kb))
                    if post is not None:
                        za, zb = post(za), post(zb)
                    put(buf, *ka, za.astype(BF))
                    put(buf, *kb, zb.astype(BF))

    def t_stage(buf, m, k, order):
        lines = [[(k, p, o) for p in range(chips)] for o in range(no)]
        for s, dist in enumerate(order):
            pair_layer(buf, lines, dist, lambda k, p, o: (wt[m, k, p, s, o, 0], wt[m, k, p, s, o, 1]))

    jobs(2, 6)
    forward(0)

    @pl.loop(0, nk)
    def _(k):
        jobs(6 + 3 * k, 9 + 3 * k)
        own_a1(k).wait()
        own_p1(k).wait()
        wait_shared(0, k)
        for r in range(1, chips):
            a1(k, r).wait_recv()
        t_stage(t1, 0, k, (2, 1))
        own_a2(k).start()
        for r in range(1, chips):
            a2(k, r).start()

    jobs(6 + 3 * nk, 2 * st)

    def wpair(i, g):
        return wl[i, g, 0], wl[i, g, 1]

    def local(i):
        return lambda k, q, o: wpair(i, gidx(k, q, o))

    def within(places, i, dist):
        for key in places:
            z = get(zm, *key)
            put(zm, *key, own_tile(masks, z, swap_rows(z, dist, br), local(i)(*key)).astype(BF))

    def over_q(k):
        return [[(k, q, o) for q in range(chips)] for o in range(no)]

    def over_o(k):
        return [[(k, q, o) for o in range(no)] for q in range(chips)]

    def places(k):
        return [(k, q, o) for q in range(chips) for o in range(no)]

    def far_local(k):
        d1(k).wait_recv()
        for key in places(k):
            put(zm, *key, own_tile(masks, get(z2, *key), get(zs1, *key), local(2)(*key)).astype(BF))
        pair_layer(zm, over_q(k), 2, local(3))
        pair_layer(zm, over_q(k), 1, local(4))
        pair_layer(zm, over_o(k), 2, local(5))
        pair_layer(zm, over_o(k), 1, local(6))
        within(places(k), 7, 2)
        within(places(k), 8, 1)

    def near_local(k):
        within(places(k), st + 4, 1)
        within(places(k), st + 5, 2)
        pair_layer(zm, over_o(k), 1, local(st + 6))
        pair_layer(zm, over_o(k), 2, local(st + 7))
        pair_layer(zm, over_q(k), 1, local(st + 8))
        pair_layer(zm, over_q(k), 2, local(st + 9))

    @pl.loop(0, nk + 1)
    def _(k):
        @pl.when(k < nk)
        def _():
            own_a2(k).wait()
            for r in range(1, chips):
                a2(k, r).wait_recv()
            d1(k).start()

        @pl.when(k == nk)
        def _():
            for r in range(1, chips):
                cross(1, r).start()
            for j in range(nk):
                own_p2(j).start()

        @pl.when(k > 0)
        def _():
            far_local(k - 1)

    @pl.loop(0, chips)
    def _(q):
        lines = [[(k, q, o) for k in range(nk)] for o in range(no)]
        pair_layer(zm, lines, 2, local(9))
        pair_layer(zm, lines, 1, local(10), lambda z: gelu(z.astype(BF).astype(F32)))
        pair_layer(zm, lines, 1, local(st + 2))
        pair_layer(zm, lines, 2, local(st + 3))

    forward(1)

    for k in range(nk):
        for r in range(1, chips):
            a1(k, r).wait_send()
            a2(k, r).wait_send()

    @pl.loop(0, nk + 1)
    def _(k):
        @pl.when(k < nk)
        def _():
            near_local(k)
            d2(k).start()

        @pl.when(k > 0)
        def _():
            j = k - 1
            d2(j).wait_recv()
            for o in range(no):
                for q in range(chips):
                    put(t1, j, q, o, own_tile(masks, get(zm, j, q, o), get(zs2, j, q, o), wpair(st + 10, gidx(j, q, o))).astype(BF))
            own_a3(j).start()
            for r in range(1, chips):
                a3(j, r).start()

    @pl.loop(0, nk)
    def _(k):
        own_a3(k).wait()
        own_p2(k).wait()
        wait_shared(1, k)
        for r in range(1, chips):
            a3(k, r).wait_recv()
        t_stage(t2, 1, k, (1, 2))
        own_a4(k).start()
        for r in range(1, chips):
            a4(k, r).start()

    @pl.loop(0, nk)
    def _(k):
        own_a4(k).wait()
        d1(k).wait_send()
        d2(k).wait_send()
        for r in range(1, chips):
            a4(k, r).wait_recv()
            a3(k, r).wait_send()
            a4(k, r).wait_send()

    for m in range(2):
        for r in range(1, chips):
            cross(m, r).wait_send()
            for j in range(1, ways):
                share(m, j, r).wait_send()


def solution(mesh):
    chips = mesh.shape["sp"] // 2

    def device_program(signal, w_first, w_second):
        rows, cols = signal.shape
        st, nb, two, br, _ = w_first.shape
        fold = LANES // br
        nk = 4
        no = nb // (chips * nk * fold)
        signal = signal.reshape(chips, no * fold, nk, br, cols)
        w1 = w_first.transpose(0, 2, 3, 4, 1)
        w2 = w_second.transpose(0, 2, 3, 4, 1)
        buf = pltpu.VMEM((nk, chips, no * fold, br, cols), BF)
        ns = nk * (chips - 1)
        fs = (nk - 1) * (chips - 1)
        pairs = [ns, chips - 1, ns, chips - 1, nk, nk, ns, ns, fs, fs]
        sems = [pltpu.SemaphoreType.DMA((n,)) for n in pairs for _ in range(2)]
        hbm = pl.BlockSpec(memory_space=pl.ANY)
        res = pl.pallas_call(
            functools.partial(kernel, chips, nk),
            out_shape=pltpu.VMEM(signal.shape, BF),
            in_specs=[hbm] * 3,
            out_specs=pl.BlockSpec(memory_space=pltpu.VMEM),
            scratch_shapes=[
                buf, buf, buf, buf, buf, buf,
                pltpu.VMEM((2 * st, nb // fold, two, br, LANES), BF),
                pltpu.VMEM((2, nk, chips, 2, no, two, br, LANES), BF),
                pltpu.VMEM((2, two, br, br, nb), BF),
                pltpu.VMEM((br, nb // fold, two * LANES), BF),
                pltpu.VMEM((nb, nb), BF),
                pltpu.VMEM((nb // fold, nb), BF),
                *sems,
                pltpu.SemaphoreType.DMA((3 * nk,)),
                pltpu.SemaphoreType.DMA((2,)),
                pltpu.SemaphoreType.DMA((3 * nk,)),
            ],
            compiler_params=pltpu.CompilerParams(
                collective_id=0, has_side_effects=True, vmem_limit_bytes=56 * 2**20
            ),
        )(signal, w1, w2)
        return res.reshape(rows, cols)

    row_spec = P(("dp", "sp"), None)
    weight_spec = P(None, "sp", None, None, None)
    return jax.shard_map(device_program, mesh=mesh, in_specs=(row_spec, weight_spec, weight_spec), out_specs=row_spec, check_vma=False)
```

```python
import functools

import jax
import jax.numpy as jnp
from jax import lax
from jax.experimental import pallas as pl
from jax.experimental.pallas import tpu as pltpu
from jax.sharding import PartitionSpec as P

MESH = pl.DeviceIdType.MESH
BF = jnp.bfloat16
F32 = jnp.float32
LANES = 128


def lane_masks(shape, br):
    lane = lax.broadcasted_iota(jnp.int32, shape, 1)
    return [(lane >= k * br) & (lane < (k + 1) * br) for k in range(LANES // br)]


def spread(w, masks):
    zero = jnp.zeros_like(w)
    return jnp.concatenate([jnp.where(m, w, zero) for m in masks], axis=0)


def pair_tile(masks, za, zb, wa, wb):
    top = jnp.concatenate([spread(wa[0], masks), spread(wa[1], masks)], axis=1)
    low = jnp.concatenate([spread(wb[1], masks), spread(wb[0], masks)], axis=1)
    lhs = jnp.concatenate([top, low], axis=0)
    rhs = jnp.concatenate([za, zb], axis=0)
    out = jnp.dot(lhs, rhs, preferred_element_type=F32)
    rows = za.shape[0]
    return out[:rows], out[rows:]


def own_tile(masks, own, other, w):
    lhs = jnp.concatenate([spread(w[0], masks), spread(w[1], masks)], axis=1)
    return jnp.dot(lhs, jnp.concatenate([own, other], axis=0), preferred_element_type=F32)


def swap_rows(z, dist, br):
    n = z.shape[0] // br
    return jnp.concatenate([z[(k ^ dist) * br:((k ^ dist) + 1) * br] for k in range(n)], axis=0)


def gelu(x):
    return 0.5 * x * (1.0 + lax.erf(x * 0.7071067811865476))


def prep_stage(nk, raw, mid, perm, sel, dst):
    two, br, _, nb = raw.shape
    fold = LANES // br
    lane = lax.broadcasted_iota(jnp.int32, (br, nb), 1) // nk % fold
    zero = jnp.zeros((br, nb), BF)
    tile = perm.shape[0] // 16
    unroll = 8

    @pl.loop(0, br // unroll)
    def _(h):
        for u in range(unroll):
            i = h * unroll + u
            rhs = jnp.concatenate([jnp.where(lane == k, raw[t, i], zero) for t in range(two) for k in range(fold)], axis=0)
            y = lax.dot_general(sel[...], rhs, (((1,), (1,)), ((), ())), preferred_element_type=F32)
            mid[i] = y.astype(BF)

    @pl.loop(0, nb // fold // tile // 2)
    def _(h):
        for u in range(2):
            g0 = (h * 2 + u) * tile
            for half in range(br // 16):
                rhs = jnp.concatenate([mid[half * 16 + v, pl.ds(pl.multiple_of(g0, tile), tile), :] for v in range(16)], axis=0)
                res = jnp.dot(perm[...], rhs, preferred_element_type=F32).astype(BF)
                for g in range(tile):
                    for t in range(two):
                        dst[g0 + g, t, half * 16:(half + 1) * 16, :] = res[g * 16:(g + 1) * 16, t * LANES:(t + 1) * LANES]


def kernel(chips, ways, sig, w1, w2, out,
           t1, z2, zs1, zm, zs2, t2, wl, wt, raw, mid, perm, sel,
           a1s, a1r, p1s, p1r, a2s, a2r, p2s, p2r, d1s, d1r, d2s, d2r, a3s, a3r, a4s, a4r, f1s, f1r, f2s, f2r,
           lsem, wsem, osem):
    d = lax.axis_index("sp")
    x = d // 2
    c = d % 2
    sib = x * 2 + (1 - c)
    group = lax.axis_index("dp")
    side = group % ways

    def mate(j):
        return {"dp": group - side + (side + j) % ways}

    br = wl.shape[3]
    fold = LANES // br
    halves, nk = z2.shape[:2]
    width = z2.shape[5]
    no = z2.shape[3] // fold

    def peer(r):
        return (x + r) % chips

    def dev(q):
        return {"sp": q * 2 + c}

    barrier = pltpu.get_barrier_semaphore()
    for r in range(1, chips):
        pl.semaphore_signal(barrier, inc=1, device_id=dev(peer(r)), device_id_type=MESH)
    pl.semaphore_signal(barrier, inc=1, device_id={"sp": sib}, device_id_type=MESH)
    for j in range(1, ways):
        pl.semaphore_signal(barrier, inc=1, device_id=mate(j), device_id_type=MESH)

    st = w1.shape[0]

    two = wl.shape[2]
    last = 2 * st - 1

    def load_w(w, stage, n):
        return pltpu.make_async_copy(w.at[stage], raw.at[n % 2], wsem.at[n % 2])

    def load_job(n):
        @pl.when(n < st)
        def _():
            load_w(w1, n, n).start()

        @pl.when((n >= st) & (n <= last))
        def _():
            load_w(w2, (n - 2) % st, n).start()

    def jobs(lo, hi):
        @pl.loop(lo, hi)
        def _(n):
            load_job(n + 1)
            load_w(w1, 0, n).wait()
            prep_stage(nk, raw.at[n % 2], mid, perm, sel, wl.at[n])

    def own_a1(k):
        return pltpu.make_async_copy(sig.at[x, :, k], t1.at[k, x], lsem.at[k])

    def wt_rows(q, k):
        return pl.ds((q * nk + k) * no, no)

    def own_p1(k):
        return pltpu.make_async_copy(wl.at[pl.ds(0, 2), wt_rows(x, k)], wt.at[0, k, x], lsem.at[nk + k])

    def own_p2(k):
        return pltpu.make_async_copy(wl.at[pl.ds(st, 2), wt_rows(x, k)], wt.at[1, k, x], lsem.at[2 * nk + k])

    load_w(w1, 0, 0).start()
    for k in range(nk):
        own_a1(k).start()
    row = lax.broadcasted_iota(jnp.int32, perm.shape, 0)
    col = lax.broadcasted_iota(jnp.int32, perm.shape, 1)
    tile = perm.shape[0] // 16
    perm[...] = (col == row % 16 * tile + row // 16).astype(F32).astype(BF)
    row = lax.broadcasted_iota(jnp.int32, sel.shape, 0)
    col = lax.broadcasted_iota(jnp.int32, sel.shape, 1)
    span = no * fold * nk
    sel[...] = (row == (col // span * nk + col % nk) * no + col // (fold * nk) % no).astype(F32).astype(BF)
    pl.semaphore_wait(barrier, chips + ways - 1)

    def slot(k, r):
        return k * (chips - 1) + (r - 1)

    def remote(src, dst, ss, rs, i, q):
        return pltpu.make_async_remote_copy(src, dst, ss.at[i], rs.at[i], device_id=dev(q), device_id_type=MESH)

    def a1(k, r):
        return remote(sig.at[peer(r), :, k], t1.at[k, x], a1s, a1r, slot(k, r), peer(r))

    def cross(m, r):
        return remote(wl.at[pl.ds(m * st, 2), wt_rows(peer(r), side)], wt.at[m, side, x], (p1s, p2s)[m], (p1r, p2r)[m], r - 1, peer(r))

    def share(m, j, r):
        ref = wt.at[m, side, peer(r)]
        i = (j - 1) * (chips - 1) + r - 1
        return pltpu.make_async_remote_copy(
            ref, ref, (f1s, f2s)[m].at[i], (f1r, f2r)[m].at[i], device_id=mate(j), device_id_type=MESH)

    def forward(m):
        for r in range(1, chips):
            cross(m, r).wait_recv()
        for j in range(1, ways):
            for r in range(1, chips):
                share(m, j, r).start()

    def wait_shared(m, k):
        @pl.when(k != side)
        def _():
            for r in range(1, chips):
                share(m, (side - k + ways) % ways, r).wait_recv()

    def lanes(h):
        return pl.ds(pl.multiple_of(h * width, width), width)

    def half_slot(h, k, r):
        return slot(h * nk + k, r)

    def a2(h, k, r):
        return remote(t1.at[k, peer(r), :, :, lanes(h)], z2.at[h, k, x], a2s, a2r, half_slot(h, k, r), peer(r))

    def a3(h, k, r):
        return remote(z2.at[h, k, peer(r)], t2.at[k, x, :, :, lanes(h)], a3s, a3r, half_slot(h, k, r), peer(r))

    def a4(k, r):
        return remote(t2.at[k, peer(r)], out.at[x, :, k], a4s, a4r, slot(k, r), peer(r))

    def sibling(src, dst, ss, rs, h, k):
        return pltpu.make_async_remote_copy(
            src.at[h, k], dst.at[h, k], ss.at[h * nk + k], rs.at[h * nk + k], device_id={"sp": sib}, device_id_type=MESH)

    def d1(h, k):
        return sibling(z2, zs1, d1s, d1r, h, k)

    def d2(h, k):
        return sibling(zm, zs2, d2s, d2r, h, k)

    def own_a2(h, k):
        return pltpu.make_async_copy(t1.at[k, x, :, :, lanes(h)], z2.at[h, k, x], osem.at[h * nk + k])

    def own_a3(h, k):
        return pltpu.make_async_copy(z2.at[h, k, x], t2.at[k, x, :, :, lanes(h)], osem.at[(halves + h) * nk + k])

    def own_a4(k):
        return pltpu.make_async_copy(t2.at[k, x], out.at[x, :, k], osem.at[2 * halves * nk + k])

    def send_a1(k):
        for r in range(1, chips):
            a1(k, r).start()

    send_a1(0)
    jobs(0, 2)
    for r in range(1, chips):
        cross(0, r).start()
    for k in range(1, nk):
        send_a1(k)
    for k in range(nk):
        own_p1(k).start()

    def get(buf, k, q, o):
        return buf[k, q, o * fold:(o + 1) * fold].reshape(fold * br, buf.shape[4])

    def put(buf, k, q, o, z):
        buf[k, q, o * fold:(o + 1) * fold] = z.reshape(fold, br, buf.shape[4])

    masks = lane_masks((br, LANES), br)

    def gidx(k, q, o):
        return (q * nk + k) * no + o

    def pair_layer(buf, lines, dist, weight, post=None):
        for line in lines:
            for a in range(len(line)):
                b = a ^ dist
                if a < b:
                    ka, kb = line[a], line[b]
                    za, zb = pair_tile(masks, get(buf, *ka), get(buf, *kb), weight(*ka), weight(*kb))
                    if post is not None:
                        za, zb = post(za), post(zb)
                    put(buf, *ka, za.astype(BF))
                    put(buf, *kb, zb.astype(BF))

    def t_stage(buf, m, k, order):
        lines = [[(k, p, o) for p in range(chips)] for o in range(no)]
        for s, dist in enumerate(order):
            pair_layer(buf, lines, dist, lambda k, p, o: (wt[m, k, p, s, o, 0], wt[m, k, p, s, o, 1]))

    jobs(2, 6)
    forward(0)

    def send_a2(h, k):
        own_a2(h, k).start()
        for r in range(1, chips):
            a2(h, k, r).start()

    @pl.loop(0, nk)
    def _(k):
        jobs(6 + 3 * k, 9 + 3 * k)
        own_a1(k).wait()
        own_p1(k).wait()
        wait_shared(0, k)
        for r in range(1, chips):
            a1(k, r).wait_recv()
        t_stage(t1, 0, k, (2, 1))
        send_a2(0, k)

    @pl.loop(1, halves)
    def _(h):
        for k in range(nk):
            send_a2(h, k)

    jobs(6 + 3 * nk, 2 * st)

    def wpair(i, g):
        return wl[i, g, 0], wl[i, g, 1]

    def local(i):
        return lambda k, q, o: wpair(i, gidx(k, q, o))

    def within(buf, places, i, dist):
        for key in places:
            z = get(buf, *key)
            put(buf, *key, own_tile(masks, z, swap_rows(z, dist, br), local(i)(*key)).astype(BF))

    def over_q(k):
        return [[(k, q, o) for q in range(chips)] for o in range(no)]

    def over_o(k):
        return [[(k, q, o) for o in range(no)] for q in range(chips)]

    def places(k):
        return [(k, q, o) for q in range(chips) for o in range(no)]

    def far_local(h, k):
        d1(h, k).wait_recv()
        buf = zm.at[h]
        for key in places(k):
            put(buf, *key, own_tile(masks, get(z2.at[h], *key), get(zs1.at[h], *key), local(2)(*key)).astype(BF))
        pair_layer(buf, over_q(k), 2, local(3))
        pair_layer(buf, over_q(k), 1, local(4))
        pair_layer(buf, over_o(k), 2, local(5))
        pair_layer(buf, over_o(k), 1, local(6))
        within(buf, places(k), 7, 2)
        within(buf, places(k), 8, 1)

    def near_local(h, k):
        buf = zm.at[h]
        within(buf, places(k), st + 4, 1)
        within(buf, places(k), st + 5, 2)
        pair_layer(buf, over_o(k), 1, local(st + 6))
        pair_layer(buf, over_o(k), 2, local(st + 7))
        pair_layer(buf, over_q(k), 1, local(st + 8))
        pair_layer(buf, over_q(k), 2, local(st + 9))

    @pl.loop(0, halves)
    def _(h):
        @pl.loop(0, nk + 1)
        def _(k):
            @pl.when(k < nk)
            def _():
                own_a2(h, k).wait()
                for r in range(1, chips):
                    a2(h, k, r).wait_recv()
                d1(h, k).start()

            @pl.when(k > 0)
            def _():
                far_local(h, k - 1)

        @pl.when(h == halves - 1)
        def _():
            for r in range(1, chips):
                cross(1, r).start()
            for j in range(nk):
                own_p2(j).start()

        @pl.loop(0, chips)
        def _(q):
            lines = [[(k, q, o) for k in range(nk)] for o in range(no)]
            buf = zm.at[h]
            pair_layer(buf, lines, 2, local(9))
            pair_layer(buf, lines, 1, local(10), lambda z: gelu(z.astype(BF).astype(F32)))
            pair_layer(buf, lines, 1, local(st + 2))
            pair_layer(buf, lines, 2, local(st + 3))

        @pl.loop(0, nk + 1)
        def _(k):
            @pl.when(k < nk)
            def _():
                near_local(h, k)
                d2(h, k).start()

            @pl.when(k > 0)
            def _():
                j = k - 1
                d1(h, j).wait_send()
                d2(h, j).wait_recv()
                for key in places(j):
                    put(z2.at[h], *key, own_tile(masks, get(zm.at[h], *key), get(zs2.at[h], *key), local(st + 10)(*key)).astype(BF))
                own_a3(h, j).start()
                for r in range(1, chips):
                    a3(h, j, r).start()

    forward(1)

    @pl.loop(0, nk)
    def _(k):
        own_p2(k).wait()
        wait_shared(1, k)
        for h in range(halves):
            own_a3(h, k).wait()
            for r in range(1, chips):
                a3(h, k, r).wait_recv()
        t_stage(t2, 1, k, (1, 2))
        own_a4(k).start()
        for r in range(1, chips):
            a4(k, r).start()

    @pl.loop(0, nk)
    def _(k):
        own_a4(k).wait()
        for r in range(1, chips):
            a1(k, r).wait_send()
            a4(k, r).wait_recv()
            a4(k, r).wait_send()
        for h in range(halves):
            d2(h, k).wait_send()
            for r in range(1, chips):
                a2(h, k, r).wait_send()
                a3(h, k, r).wait_send()

    for m in range(2):
        for r in range(1, chips):
            cross(m, r).wait_send()
            for j in range(1, ways):
                share(m, j, r).wait_send()


def solution(mesh):
    chips = mesh.shape["sp"] // 2

    def device_program(signal, w_first, w_second):
        rows, cols = signal.shape
        st, nb, two, br, _ = w_first.shape
        fold = LANES // br
        nk = 4
        no = nb // (chips * nk * fold)
        signal = signal.reshape(chips, no * fold, nk, br, cols)
        w1 = w_first.transpose(0, 2, 3, 4, 1)
        w2 = w_second.transpose(0, 2, 3, 4, 1)
        buf = pltpu.VMEM((nk, chips, no * fold, br, cols), BF)
        half = pltpu.VMEM((cols // LANES, nk, chips, no * fold, br, LANES), BF)
        ns = nk * (chips - 1)
        hs = cols // LANES
        fs = (nk - 1) * (chips - 1)
        pairs = [ns, chips - 1, hs * ns, chips - 1, hs * nk, hs * nk, hs * ns, ns, fs, fs]
        sems = [pltpu.SemaphoreType.DMA((n,)) for n in pairs for _ in range(2)]
        hbm = pl.BlockSpec(memory_space=pl.ANY)
        res = pl.pallas_call(
            functools.partial(kernel, chips, nk),
            out_shape=pltpu.VMEM(signal.shape, BF),
            in_specs=[hbm] * 3,
            out_specs=pl.BlockSpec(memory_space=pltpu.VMEM),
            scratch_shapes=[
                buf, half, half, half, half, buf,
                pltpu.VMEM((2 * st, nb // fold, two, br, LANES), BF),
                pltpu.VMEM((2, nk, chips, 2, no, two, br, LANES), BF),
                pltpu.VMEM((2, two, br, br, nb), BF),
                pltpu.VMEM((br, nb // fold, two * LANES), BF),
                pltpu.VMEM((nb, nb), BF),
                pltpu.VMEM((nb // fold, nb), BF),
                *sems,
                pltpu.SemaphoreType.DMA((3 * nk,)),
                pltpu.SemaphoreType.DMA((2,)),
                pltpu.SemaphoreType.DMA(((2 * hs + 1) * nk,)),
            ],
            compiler_params=pltpu.CompilerParams(
                collective_id=0, has_side_effects=True, vmem_limit_bytes=56 * 2**20
            ),
        )(signal, w1, w2)
        return res.reshape(rows, cols)

    row_spec = P(("dp", "sp"), None)
    weight_spec = P(None, "sp", None, None, None)
    return jax.shard_map(device_program, mesh=mesh, in_specs=(row_spec, weight_spec, weight_spec), out_specs=row_spec, check_vma=False)
```

```python
import functools

import jax
import jax.numpy as jnp
from jax import lax
from jax.experimental import pallas as pl
from jax.experimental.pallas import tpu as pltpu
from jax.sharding import PartitionSpec as P

MESH = pl.DeviceIdType.MESH
BF = jnp.bfloat16
F32 = jnp.float32
LANES = 128


def lane_masks(shape, br):
    lane = lax.broadcasted_iota(jnp.int32, shape, 1)
    return [(lane >= k * br) & (lane < (k + 1) * br) for k in range(LANES // br)]


def spread(w, masks):
    zero = jnp.zeros_like(w)
    return jnp.concatenate([jnp.where(m, w, zero) for m in masks], axis=0)


def pair_tile(masks, za, zb, wa, wb):
    top = jnp.concatenate([spread(wa[0], masks), spread(wa[1], masks)], axis=1)
    low = jnp.concatenate([spread(wb[1], masks), spread(wb[0], masks)], axis=1)
    lhs = jnp.concatenate([top, low], axis=0)
    rhs = jnp.concatenate([za, zb], axis=0)
    out = jnp.dot(lhs, rhs, preferred_element_type=F32)
    rows = za.shape[0]
    return out[:rows], out[rows:]


def own_tile(masks, own, other, w):
    lhs = jnp.concatenate([spread(w[0], masks), spread(w[1], masks)], axis=1)
    return jnp.dot(lhs, jnp.concatenate([own, other], axis=0), preferred_element_type=F32)


def swap_rows(z, dist, br):
    n = z.shape[0] // br
    return jnp.concatenate([z[(k ^ dist) * br:((k ^ dist) + 1) * br] for k in range(n)], axis=0)


def gelu(x):
    return 0.5 * x * (1.0 + lax.erf(x * 0.7071067811865476))


def prep_stage(nk, raw, mid, perm, sel, dst):
    two, br, _, nb = raw.shape
    fold = LANES // br
    lane = lax.broadcasted_iota(jnp.int32, (br, nb), 1) // nk % fold
    zero = jnp.zeros((br, nb), BF)
    tile = perm.shape[0] // 16
    unroll = 8

    @pl.loop(0, br // unroll)
    def _(h):
        for u in range(unroll):
            i = h * unroll + u
            rhs = jnp.concatenate([jnp.where(lane == k, raw[t, i], zero) for t in range(two) for k in range(fold)], axis=0)
            y = lax.dot_general(sel[...], rhs, (((1,), (1,)), ((), ())), preferred_element_type=F32)
            mid[i] = y.astype(BF)

    @pl.loop(0, nb // fold // tile // 2)
    def _(h):
        for u in range(2):
            g0 = (h * 2 + u) * tile
            for half in range(br // 16):
                rhs = jnp.concatenate([mid[half * 16 + v, pl.ds(pl.multiple_of(g0, tile), tile), :] for v in range(16)], axis=0)
                res = jnp.dot(perm[...], rhs, preferred_element_type=F32).astype(BF)
                for g in range(tile):
                    for t in range(two):
                        dst[g0 + g, t, half * 16:(half + 1) * 16, :] = res[g * 16:(g + 1) * 16, t * LANES:(t + 1) * LANES]


def kernel(chips, ways, sig, w1, w2, out,
           t1, z2, zs1, zm, zs2, t2, wl, wt, raw, mid, perm, sel,
           a1s, a1r, p1s, p1r, a2s, a2r, p2s, p2r, d1s, d1r, d2s, d2r, a3s, a3r, a4s, a4r, f1s, f1r, f2s, f2r,
           lsem, wsem, osem):
    d = lax.axis_index("sp")
    x = d // 2
    c = d % 2
    sib = x * 2 + (1 - c)
    group = lax.axis_index("dp")
    side = group % ways

    def mate(j):
        return {"dp": group - side + (side + j) % ways}

    br = wl.shape[3]
    fold = LANES // br
    halves, nk = z2.shape[:2]
    width = z2.shape[5]
    no = z2.shape[3] // fold

    def peer(r):
        return (x + r) % chips

    def dev(q):
        return {"sp": q * 2 + c}

    barrier = pltpu.get_barrier_semaphore()
    for r in range(1, chips):
        pl.semaphore_signal(barrier, inc=1, device_id=dev(peer(r)), device_id_type=MESH)
    pl.semaphore_signal(barrier, inc=1, device_id={"sp": sib}, device_id_type=MESH)
    for j in range(1, ways):
        pl.semaphore_signal(barrier, inc=1, device_id=mate(j), device_id_type=MESH)

    st = w1.shape[0]

    two = wl.shape[2]
    last = 2 * st - 1

    def load_w(w, stage, n):
        return pltpu.make_async_copy(w.at[stage], raw.at[n % 2], wsem.at[n % 2])

    def load_job(n):
        @pl.when(n < st)
        def _():
            load_w(w1, n, n).start()

        @pl.when((n >= st) & (n <= last))
        def _():
            load_w(w2, (n - 2) % st, n).start()

    def jobs(lo, hi):
        @pl.loop(lo, hi)
        def _(n):
            load_job(n + 1)
            load_w(w1, 0, n).wait()
            prep_stage(nk, raw.at[n % 2], mid, perm, sel, wl.at[n])

    def own_a1(k):
        return pltpu.make_async_copy(sig.at[x, :, k], t1.at[k, x], lsem.at[k])

    def wt_rows(q, k):
        return pl.ds((q * nk + k) * no, no)

    def own_p1(k):
        return pltpu.make_async_copy(wl.at[pl.ds(0, 2), wt_rows(x, k)], wt.at[0, k, x], lsem.at[nk + k])

    def own_p2(k):
        return pltpu.make_async_copy(wl.at[pl.ds(st, 2), wt_rows(x, k)], wt.at[1, k, x], lsem.at[2 * nk + k])

    load_w(w1, 0, 0).start()
    for k in range(nk):
        own_a1(k).start()
    pl.semaphore_wait(barrier, chips + ways - 1)

    def slot(k, r):
        return k * (chips - 1) + (r - 1)

    def remote(src, dst, ss, rs, i, q):
        return pltpu.make_async_remote_copy(src, dst, ss.at[i], rs.at[i], device_id=dev(q), device_id_type=MESH)

    def a1(k, r):
        return remote(sig.at[peer(r), :, k], t1.at[k, x], a1s, a1r, slot(k, r), peer(r))

    def cross(m, r):
        return remote(wl.at[pl.ds(m * st, 2), wt_rows(peer(r), side)], wt.at[m, side, x], (p1s, p2s)[m], (p1r, p2r)[m], r - 1, peer(r))

    def share(m, j, r):
        ref = wt.at[m, side, peer(r)]
        i = (j - 1) * (chips - 1) + r - 1
        return pltpu.make_async_remote_copy(
            ref, ref, (f1s, f2s)[m].at[i], (f1r, f2r)[m].at[i], device_id=mate(j), device_id_type=MESH)

    def forward(m):
        for r in range(1, chips):
            cross(m, r).wait_recv()
        for j in range(1, ways):
            for r in range(1, chips):
                share(m, j, r).start()

    def wait_shared(m, k):
        @pl.when(k != side)
        def _():
            for r in range(1, chips):
                share(m, (side - k + ways) % ways, r).wait_recv()

    def lanes(h):
        return pl.ds(pl.multiple_of(h * width, width), width)

    def half_slot(h, k, r):
        return slot(h * nk + k, r)

    def a2(h, k, r):
        return remote(t1.at[k, peer(r), :, :, lanes(h)], z2.at[h, k, x], a2s, a2r, half_slot(h, k, r), peer(r))

    def a3(h, k, r):
        return remote(z2.at[h, k, peer(r)], t2.at[k, x, :, :, lanes(h)], a3s, a3r, half_slot(h, k, r), peer(r))

    def a4(k, r):
        return remote(t2.at[k, peer(r)], out.at[x, :, k], a4s, a4r, slot(k, r), peer(r))

    def sibling(src, dst, ss, rs, h, k):
        return pltpu.make_async_remote_copy(
            src.at[h, k], dst.at[h, k], ss.at[h * nk + k], rs.at[h * nk + k], device_id={"sp": sib}, device_id_type=MESH)

    def d1(h, k):
        return sibling(z2, zs1, d1s, d1r, h, k)

    def d2(h, k):
        return sibling(zm, zs2, d2s, d2r, h, k)

    def own_a2(h, k):
        return pltpu.make_async_copy(t1.at[k, x, :, :, lanes(h)], z2.at[h, k, x], osem.at[h * nk + k])

    def own_a3(h, k):
        return pltpu.make_async_copy(z2.at[h, k, x], t2.at[k, x, :, :, lanes(h)], osem.at[(halves + h) * nk + k])

    def own_a4(k):
        return pltpu.make_async_copy(t2.at[k, x], out.at[x, :, k], osem.at[2 * halves * nk + k])

    def send_a1(k):
        for r in range(1, chips):
            a1(k, r).start()

    send_a1(0)
    row = lax.broadcasted_iota(jnp.int32, perm.shape, 0)
    col = lax.broadcasted_iota(jnp.int32, perm.shape, 1)
    tile = perm.shape[0] // 16
    perm[...] = (col == row % 16 * tile + row // 16).astype(F32).astype(BF)
    row = lax.broadcasted_iota(jnp.int32, sel.shape, 0)
    col = lax.broadcasted_iota(jnp.int32, sel.shape, 1)
    span = no * fold * nk
    sel[...] = (row == (col // span * nk + col % nk) * no + col // (fold * nk) % no).astype(F32).astype(BF)
    jobs(0, 2)
    for r in range(1, chips):
        cross(0, r).start()
    for k in range(1, nk):
        send_a1(k)
    for k in range(nk):
        own_p1(k).start()

    def get(buf, k, q, o):
        return buf[k, q, o * fold:(o + 1) * fold].reshape(fold * br, buf.shape[4])

    def put(buf, k, q, o, z):
        buf[k, q, o * fold:(o + 1) * fold] = z.reshape(fold, br, buf.shape[4])

    masks = lane_masks((br, LANES), br)

    def gidx(k, q, o):
        return (q * nk + k) * no + o

    def pair_layer(buf, lines, dist, weight, post=None):
        for line in lines:
            for a in range(len(line)):
                b = a ^ dist
                if a < b:
                    ka, kb = line[a], line[b]
                    za, zb = pair_tile(masks, get(buf, *ka), get(buf, *kb), weight(*ka), weight(*kb))
                    if post is not None:
                        za, zb = post(za), post(zb)
                    put(buf, *ka, za.astype(BF))
                    put(buf, *kb, zb.astype(BF))

    def t_stage(buf, m, k, order):
        lines = [[(k, p, o) for p in range(chips)] for o in range(no)]
        for s, dist in enumerate(order):
            pair_layer(buf, lines, dist, lambda k, p, o: (wt[m, k, p, s, o, 0], wt[m, k, p, s, o, 1]))

    jobs(2, 6)
    forward(0)

    def send_a2(h, k):
        own_a2(h, k).start()
        for r in range(1, chips):
            a2(h, k, r).start()

    @pl.loop(0, nk)
    def _(k):
        jobs(6 + 3 * k, 9 + 3 * k)
        own_a1(k).wait()
        own_p1(k).wait()
        wait_shared(0, k)
        for r in range(1, chips):
            a1(k, r).wait_recv()
        t_stage(t1, 0, k, (2, 1))
        send_a2(0, k)

    for r in range(1, chips):
        cross(1, r).start()
    for k in range(nk):
        own_p2(k).start()

    @pl.loop(1, halves)
    def _(h):
        for k in range(nk):
            send_a2(h, k)

    jobs(6 + 3 * nk, 2 * st)

    def wpair(i, g):
        return wl[i, g, 0], wl[i, g, 1]

    def local(i):
        return lambda k, q, o: wpair(i, gidx(k, q, o))

    def within(buf, places, i, dist):
        for key in places:
            z = get(buf, *key)
            put(buf, *key, own_tile(masks, z, swap_rows(z, dist, br), local(i)(*key)).astype(BF))

    def over_q(k):
        return [[(k, q, o) for q in range(chips)] for o in range(no)]

    def over_o(k):
        return [[(k, q, o) for o in range(no)] for q in range(chips)]

    def places(k):
        return [(k, q, o) for q in range(chips) for o in range(no)]

    def far_local(h, k):
        d1(h, k).wait_recv()
        buf = zm.at[h]
        for key in places(k):
            put(buf, *key, own_tile(masks, get(z2.at[h], *key), get(zs1.at[h], *key), local(2)(*key)).astype(BF))
        pair_layer(buf, over_q(k), 2, local(3))
        pair_layer(buf, over_q(k), 1, local(4))
        pair_layer(buf, over_o(k), 2, local(5))
        pair_layer(buf, over_o(k), 1, local(6))
        within(buf, places(k), 7, 2)
        within(buf, places(k), 8, 1)

    def near_local(h, k):
        buf = zm.at[h]
        within(buf, places(k), st + 4, 1)
        within(buf, places(k), st + 5, 2)
        pair_layer(buf, over_o(k), 1, local(st + 6))
        pair_layer(buf, over_o(k), 2, local(st + 7))
        pair_layer(buf, over_q(k), 1, local(st + 8))
        pair_layer(buf, over_q(k), 2, local(st + 9))

    @pl.loop(0, halves)
    def _(h):
        @pl.loop(0, nk + 1)
        def _(k):
            @pl.when(k < nk)
            def _():
                own_a2(h, k).wait()
                for r in range(1, chips):
                    a2(h, k, r).wait_recv()
                d1(h, k).start()

            @pl.when(k > 0)
            def _():
                far_local(h, k - 1)

        @pl.loop(0, chips)
        def _(q):
            lines = [[(k, q, o) for k in range(nk)] for o in range(no)]
            buf = zm.at[h]
            pair_layer(buf, lines, 2, local(9))
            pair_layer(buf, lines, 1, local(10), lambda z: gelu(z.astype(BF).astype(F32)))
            pair_layer(buf, lines, 1, local(st + 2))
            pair_layer(buf, lines, 2, local(st + 3))

        @pl.when(h == 0)
        def _():
            forward(1)

        @pl.loop(0, nk + 1)
        def _(k):
            @pl.when(k < nk)
            def _():
                near_local(h, k)
                d2(h, k).start()

            @pl.when(k > 0)
            def _():
                j = k - 1
                d1(h, j).wait_send()
                d2(h, j).wait_recv()
                for key in places(j):
                    put(z2.at[h], *key, own_tile(masks, get(zm.at[h], *key), get(zs2.at[h], *key), local(st + 10)(*key)).astype(BF))
                own_a3(h, j).start()
                for r in range(1, chips):
                    a3(h, j, r).start()

    @pl.loop(0, nk)
    def _(k):
        own_p2(k).wait()
        wait_shared(1, k)
        for h in range(halves):
            own_a3(h, k).wait()
            for r in range(1, chips):
                a3(h, k, r).wait_recv()
        t_stage(t2, 1, k, (1, 2))
        own_a4(k).start()
        for r in range(1, chips):
            a4(k, r).start()

    @pl.loop(0, nk)
    def _(k):
        own_a4(k).wait()
        for r in range(1, chips):
            a1(k, r).wait_send()
            a4(k, r).wait_recv()
            a4(k, r).wait_send()
        for h in range(halves):
            d2(h, k).wait_send()
            for r in range(1, chips):
                a2(h, k, r).wait_send()
                a3(h, k, r).wait_send()

    for m in range(2):
        for r in range(1, chips):
            cross(m, r).wait_send()
            for j in range(1, ways):
                share(m, j, r).wait_send()


def solution(mesh):
    chips = mesh.shape["sp"] // 2

    def device_program(signal, w_first, w_second):
        rows, cols = signal.shape
        st, nb, two, br, _ = w_first.shape
        fold = LANES // br
        nk = 4
        no = nb // (chips * nk * fold)
        signal = signal.reshape(chips, no * fold, nk, br, cols)
        w1 = w_first.transpose(0, 2, 3, 4, 1)
        w2 = w_second.transpose(0, 2, 3, 4, 1)
        buf = pltpu.VMEM((nk, chips, no * fold, br, cols), BF)
        half = pltpu.VMEM((cols // LANES, nk, chips, no * fold, br, LANES), BF)
        ns = nk * (chips - 1)
        hs = cols // LANES
        fs = (nk - 1) * (chips - 1)
        pairs = [ns, chips - 1, hs * ns, chips - 1, hs * nk, hs * nk, hs * ns, ns, fs, fs]
        sems = [pltpu.SemaphoreType.DMA((n,)) for n in pairs for _ in range(2)]
        hbm = pl.BlockSpec(memory_space=pl.ANY)
        res = pl.pallas_call(
            functools.partial(kernel, chips, nk),
            out_shape=pltpu.VMEM(signal.shape, BF),
            in_specs=[hbm] * 3,
            out_specs=pl.BlockSpec(memory_space=pltpu.VMEM),
            scratch_shapes=[
                buf, half, half, half, half, buf,
                pltpu.VMEM((2 * st, nb // fold, two, br, LANES), BF),
                pltpu.VMEM((2, nk, chips, 2, no, two, br, LANES), BF),
                pltpu.VMEM((2, two, br, br, nb), BF),
                pltpu.VMEM((br, nb // fold, two * LANES), BF),
                pltpu.VMEM((nb, nb), BF),
                pltpu.VMEM((nb // fold, nb), BF),
                *sems,
                pltpu.SemaphoreType.DMA((3 * nk,)),
                pltpu.SemaphoreType.DMA((2,)),
                pltpu.SemaphoreType.DMA(((2 * hs + 1) * nk,)),
            ],
            compiler_params=pltpu.CompilerParams(
                collective_id=0, has_side_effects=True, vmem_limit_bytes=56 * 2**20
            ),
        )(signal, w1, w2)
        return res.reshape(rows, cols)

    row_spec = P(("dp", "sp"), None)
    weight_spec = P(None, "sp", None, None, None)
    return jax.shard_map(device_program, mesh=mesh, in_specs=(row_spec, weight_spec, weight_spec), out_specs=row_spec, check_vma=False)
```

```python
import functools

import jax
import jax.numpy as jnp
from jax import lax
from jax.experimental import pallas as pl
from jax.experimental.pallas import tpu as pltpu
from jax.sharding import PartitionSpec as P

MESH = pl.DeviceIdType.MESH
BF = jnp.bfloat16
F32 = jnp.float32
LANES = 128


def lane_masks(shape, br):
    lane = lax.broadcasted_iota(jnp.int32, shape, 1)
    return [(lane >= k * br) & (lane < (k + 1) * br) for k in range(LANES // br)]


def spread(w, masks):
    zero = jnp.zeros_like(w)
    return jnp.concatenate([jnp.where(m, w, zero) for m in masks], axis=0)


def pair_tile(masks, za, zb, wa, wb):
    top = jnp.concatenate([spread(wa[0], masks), spread(wa[1], masks)], axis=1)
    low = jnp.concatenate([spread(wb[1], masks), spread(wb[0], masks)], axis=1)
    lhs = jnp.concatenate([top, low], axis=0)
    rhs = jnp.concatenate([za, zb], axis=0)
    out = jnp.dot(lhs, rhs, preferred_element_type=F32)
    rows = za.shape[0]
    return out[:rows], out[rows:]


def own_tile(masks, own, other, w):
    lhs = jnp.concatenate([spread(w[0], masks), spread(w[1], masks)], axis=1)
    return jnp.dot(lhs, jnp.concatenate([own, other], axis=0), preferred_element_type=F32)


def swap_rows(z, dist, br):
    n = z.shape[0] // br
    return jnp.concatenate([z[(k ^ dist) * br:((k ^ dist) + 1) * br] for k in range(n)], axis=0)


def gelu(x):
    return 0.5 * x * (1.0 + lax.erf(x * 0.7071067811865476))


def prep_stage(nk, raw, mid, perm, sel, dst):
    two, br, _, nb = raw.shape
    fold = LANES // br
    lane = lax.broadcasted_iota(jnp.int32, (br, nb), 1) // nk % fold
    zero = jnp.zeros((br, nb), BF)
    tile = perm.shape[0] // 16
    unroll = 8

    @pl.loop(0, br // unroll)
    def _(h):
        for u in range(unroll):
            i = h * unroll + u
            rhs = jnp.concatenate([jnp.where(lane == k, raw[t, i], zero) for t in range(two) for k in range(fold)], axis=0)
            y = lax.dot_general(sel[...], rhs, (((1,), (1,)), ((), ())), preferred_element_type=F32)
            mid[i] = y.astype(BF)

    @pl.loop(0, nb // fold // tile // 2)
    def _(h):
        for u in range(2):
            g0 = (h * 2 + u) * tile
            for half in range(br // 16):
                rhs = jnp.concatenate([mid[half * 16 + v, pl.ds(pl.multiple_of(g0, tile), tile), :] for v in range(16)], axis=0)
                res = jnp.dot(perm[...], rhs, preferred_element_type=F32).astype(BF)
                for g in range(tile):
                    for t in range(two):
                        dst[g0 + g, t, half * 16:(half + 1) * 16, :] = res[g * 16:(g + 1) * 16, t * LANES:(t + 1) * LANES]


def kernel(chips, ways, sig, w1, w2, out,
           t1, z2, zs1, zm, zs2, t2, wl, wt, raw, mid, perm, sel,
           a1s, a1r, p1s, p1r, a2s, a2r, p2s, p2r, d1s, d1r, d2s, d2r, a3s, a3r, a4s, a4r, f1s, f1r, f2s, f2r,
           lsem, wsem, osem):
    d = lax.axis_index("sp")
    x = d // 2
    c = d % 2
    sib = x * 2 + (1 - c)
    group = lax.axis_index("dp")
    side = group % ways

    def mate(j):
        return {"dp": group - side + (side + j) % ways}

    br = wl.shape[3]
    fold = LANES // br
    halves, nk = z2.shape[:2]
    width = z2.shape[5]
    no = z2.shape[3] // fold

    def peer(r):
        return (x + r) % chips

    order = sorted(range(1, chips), key=lambda r: -min(r, chips - r))

    def dev(q):
        return {"sp": q * 2 + c}

    barrier = pltpu.get_barrier_semaphore()
    for r in range(1, chips):
        pl.semaphore_signal(barrier, inc=1, device_id=dev(peer(r)), device_id_type=MESH)
    pl.semaphore_signal(barrier, inc=1, device_id={"sp": sib}, device_id_type=MESH)
    for j in range(1, ways):
        pl.semaphore_signal(barrier, inc=1, device_id=mate(j), device_id_type=MESH)

    st = w1.shape[0]

    two = wl.shape[2]
    last = 2 * st - 1

    def load_w(w, stage, n):
        return pltpu.make_async_copy(w.at[stage], raw.at[n % 2], wsem.at[n % 2])

    def load_job(n):
        @pl.when(n < st)
        def _():
            load_w(w1, n, n).start()

        @pl.when((n >= st) & (n <= last))
        def _():
            load_w(w2, (n - 2) % st, n).start()

    def jobs(lo, hi):
        @pl.loop(lo, hi)
        def _(n):
            load_job(n + 1)
            load_w(w1, 0, n).wait()
            prep_stage(nk, raw.at[n % 2], mid, perm, sel, wl.at[n])

    def own_a1(k):
        return pltpu.make_async_copy(sig.at[x, :, k], t1.at[k, x], lsem.at[k])

    def wt_rows(q, k):
        return pl.ds((q * nk + k) * no, no)

    def own_p1(k):
        return pltpu.make_async_copy(wl.at[pl.ds(0, 2), wt_rows(x, k)], wt.at[0, k, x], lsem.at[nk + k])

    def own_p2(k):
        return pltpu.make_async_copy(wl.at[pl.ds(st, 2), wt_rows(x, k)], wt.at[1, k, x], lsem.at[2 * nk + k])

    load_w(w1, 0, 0).start()
    for k in range(nk):
        own_a1(k).start()
    pl.semaphore_wait(barrier, chips + ways - 1)

    def slot(k, r):
        return k * (chips - 1) + (r - 1)

    def remote(src, dst, ss, rs, i, q):
        return pltpu.make_async_remote_copy(src, dst, ss.at[i], rs.at[i], device_id=dev(q), device_id_type=MESH)

    def a1(k, r):
        return remote(sig.at[peer(r), :, k], t1.at[k, x], a1s, a1r, slot(k, r), peer(r))

    def cross(m, r):
        return remote(wl.at[pl.ds(m * st, 2), wt_rows(peer(r), side)], wt.at[m, side, x], (p1s, p2s)[m], (p1r, p2r)[m], r - 1, peer(r))

    def share(m, j, r):
        ref = wt.at[m, side, peer(r)]
        i = (j - 1) * (chips - 1) + r - 1
        return pltpu.make_async_remote_copy(
            ref, ref, (f1s, f2s)[m].at[i], (f1r, f2r)[m].at[i], device_id=mate(j), device_id_type=MESH)

    def forward(m):
        for r in range(1, chips):
            cross(m, r).wait_recv()
        for j in range(1, ways):
            for r in range(1, chips):
                share(m, j, r).start()

    def wait_shared(m, k):
        @pl.when(k != side)
        def _():
            for r in range(1, chips):
                share(m, (side - k + ways) % ways, r).wait_recv()

    def lanes(h):
        return pl.ds(pl.multiple_of(h * width, width), width)

    def half_slot(h, k, r):
        return slot(h * nk + k, r)

    def a2(h, k, r):
        return remote(t1.at[k, peer(r), :, :, lanes(h)], z2.at[h, k, x], a2s, a2r, half_slot(h, k, r), peer(r))

    def a3(h, k, r):
        return remote(z2.at[h, k, peer(r)], t2.at[k, x, :, :, lanes(h)], a3s, a3r, half_slot(h, k, r), peer(r))

    def a4(k, r):
        return remote(t2.at[k, peer(r)], out.at[x, :, k], a4s, a4r, slot(k, r), peer(r))

    def sibling(src, dst, ss, rs, h, k):
        return pltpu.make_async_remote_copy(
            src.at[h, k], dst.at[h, k], ss.at[h * nk + k], rs.at[h * nk + k], device_id={"sp": sib}, device_id_type=MESH)

    def d1(h, k):
        return sibling(z2, zs1, d1s, d1r, h, k)

    def d2(h, k):
        return sibling(zm, zs2, d2s, d2r, h, k)

    def own_a2(h, k):
        return pltpu.make_async_copy(t1.at[k, x, :, :, lanes(h)], z2.at[h, k, x], osem.at[h * nk + k])

    def own_a3(h, k):
        return pltpu.make_async_copy(z2.at[h, k, x], t2.at[k, x, :, :, lanes(h)], osem.at[(halves + h) * nk + k])

    def own_a4(k):
        return pltpu.make_async_copy(t2.at[k, x], out.at[x, :, k], osem.at[2 * halves * nk + k])

    def send_a1(k):
        for r in order:
            a1(k, r).start()

    send_a1(0)
    row = lax.broadcasted_iota(jnp.int32, perm.shape, 0)
    col = lax.broadcasted_iota(jnp.int32, perm.shape, 1)
    tile = perm.shape[0] // 16
    perm[...] = (col == row % 16 * tile + row // 16).astype(F32).astype(BF)
    row = lax.broadcasted_iota(jnp.int32, sel.shape, 0)
    col = lax.broadcasted_iota(jnp.int32, sel.shape, 1)
    span = no * fold * nk
    sel[...] = (row == (col // span * nk + col % nk) * no + col // (fold * nk) % no).astype(F32).astype(BF)
    jobs(0, 2)
    for r in range(1, chips):
        cross(0, r).start()
    for k in range(1, nk):
        send_a1(k)
    for k in range(nk):
        own_p1(k).start()

    def get(buf, k, q, o):
        return buf[k, q, o * fold:(o + 1) * fold].reshape(fold * br, buf.shape[4])

    def put(buf, k, q, o, z):
        buf[k, q, o * fold:(o + 1) * fold] = z.reshape(fold, br, buf.shape[4])

    masks = lane_masks((br, LANES), br)

    def gidx(k, q, o):
        return (q * nk + k) * no + o

    def pair_layer(buf, lines, dist, weight, post=None):
        for line in lines:
            for a in range(len(line)):
                b = a ^ dist
                if a < b:
                    ka, kb = line[a], line[b]
                    za, zb = pair_tile(masks, get(buf, *ka), get(buf, *kb), weight(*ka), weight(*kb))
                    if post is not None:
                        za, zb = post(za), post(zb)
                    put(buf, *ka, za.astype(BF))
                    put(buf, *kb, zb.astype(BF))

    def t_stage(buf, m, k, order):
        lines = [[(k, p, o) for p in range(chips)] for o in range(no)]
        for s, dist in enumerate(order):
            pair_layer(buf, lines, dist, lambda k, p, o: (wt[m, k, p, s, o, 0], wt[m, k, p, s, o, 1]))

    jobs(2, 6)
    forward(0)

    def send_a2(h, k):
        own_a2(h, k).start()
        for r in order:
            a2(h, k, r).start()

    @pl.loop(0, nk)
    def _(k):
        jobs(6 + 3 * k, 9 + 3 * k)
        own_a1(k).wait()
        own_p1(k).wait()
        wait_shared(0, k)
        for r in range(1, chips):
            a1(k, r).wait_recv()
        t_stage(t1, 0, k, (2, 1))
        send_a2(0, k)

    for r in range(1, chips):
        cross(1, r).start()
    for k in range(nk):
        own_p2(k).start()

    @pl.loop(1, halves)
    def _(h):
        for k in range(nk):
            send_a2(h, k)

    jobs(6 + 3 * nk, 2 * st)

    def wpair(i, g):
        return wl[i, g, 0], wl[i, g, 1]

    def local(i):
        return lambda k, q, o: wpair(i, gidx(k, q, o))

    def within(buf, places, i, dist):
        for key in places:
            z = get(buf, *key)
            put(buf, *key, own_tile(masks, z, swap_rows(z, dist, br), local(i)(*key)).astype(BF))

    def over_q(k):
        return [[(k, q, o) for q in range(chips)] for o in range(no)]

    def over_o(k):
        return [[(k, q, o) for o in range(no)] for q in range(chips)]

    def places(k):
        return [(k, q, o) for q in range(chips) for o in range(no)]

    def far_local(h, k):
        d1(h, k).wait_recv()
        buf = zm.at[h]
        for key in places(k):
            put(buf, *key, own_tile(masks, get(z2.at[h], *key), get(zs1.at[h], *key), local(2)(*key)).astype(BF))
        pair_layer(buf, over_q(k), 2, local(3))
        pair_layer(buf, over_q(k), 1, local(4))
        pair_layer(buf, over_o(k), 2, local(5))
        pair_layer(buf, over_o(k), 1, local(6))
        within(buf, places(k), 7, 2)
        within(buf, places(k), 8, 1)

    def near_local(h, k):
        buf = zm.at[h]
        within(buf, places(k), st + 4, 1)
        within(buf, places(k), st + 5, 2)
        pair_layer(buf, over_o(k), 1, local(st + 6))
        pair_layer(buf, over_o(k), 2, local(st + 7))
        pair_layer(buf, over_q(k), 1, local(st + 8))
        pair_layer(buf, over_q(k), 2, local(st + 9))

    @pl.loop(0, halves)
    def _(h):
        @pl.loop(0, nk + 1)
        def _(k):
            @pl.when(k < nk)
            def _():
                own_a2(h, k).wait()
                for r in range(1, chips):
                    a2(h, k, r).wait_recv()
                d1(h, k).start()

            @pl.when(k > 0)
            def _():
                far_local(h, k - 1)

        @pl.loop(0, chips)
        def _(q):
            lines = [[(k, q, o) for k in range(nk)] for o in range(no)]
            buf = zm.at[h]
            pair_layer(buf, lines, 2, local(9))
            pair_layer(buf, lines, 1, local(10), lambda z: gelu(z.astype(BF).astype(F32)))
            pair_layer(buf, lines, 1, local(st + 2))
            pair_layer(buf, lines, 2, local(st + 3))

        @pl.when(h == 0)
        def _():
            forward(1)

        @pl.loop(0, nk + 1)
        def _(k):
            @pl.when(k < nk)
            def _():
                near_local(h, k)
                d2(h, k).start()

            @pl.when(k > 0)
            def _():
                j = k - 1
                d1(h, j).wait_send()
                d2(h, j).wait_recv()
                for key in places(j):
                    put(z2.at[h], *key, own_tile(masks, get(zm.at[h], *key), get(zs2.at[h], *key), local(st + 10)(*key)).astype(BF))
                own_a3(h, j).start()
                for r in order:
                    a3(h, j, r).start()

    @pl.loop(0, nk)
    def _(k):
        own_p2(k).wait()
        wait_shared(1, k)
        for h in range(halves):
            own_a3(h, k).wait()
            for r in range(1, chips):
                a3(h, k, r).wait_recv()
        t_stage(t2, 1, k, (1, 2))
        own_a4(k).start()
        for r in order:
            a4(k, r).start()

    @pl.loop(0, nk)
    def _(k):
        own_a4(k).wait()
        for r in range(1, chips):
            a1(k, r).wait_send()
            a4(k, r).wait_recv()
            a4(k, r).wait_send()
        for h in range(halves):
            d2(h, k).wait_send()
            for r in range(1, chips):
                a2(h, k, r).wait_send()
                a3(h, k, r).wait_send()

    for m in range(2):
        for r in range(1, chips):
            cross(m, r).wait_send()
            for j in range(1, ways):
                share(m, j, r).wait_send()


def solution(mesh):
    chips = mesh.shape["sp"] // 2

    def device_program(signal, w_first, w_second):
        rows, cols = signal.shape
        st, nb, two, br, _ = w_first.shape
        fold = LANES // br
        nk = 4
        no = nb // (chips * nk * fold)
        signal = signal.reshape(chips, no * fold, nk, br, cols)
        w1 = w_first.transpose(0, 2, 3, 4, 1)
        w2 = w_second.transpose(0, 2, 3, 4, 1)
        buf = pltpu.VMEM((nk, chips, no * fold, br, cols), BF)
        half = pltpu.VMEM((cols // LANES, nk, chips, no * fold, br, LANES), BF)
        ns = nk * (chips - 1)
        hs = cols // LANES
        fs = (nk - 1) * (chips - 1)
        pairs = [ns, chips - 1, hs * ns, chips - 1, hs * nk, hs * nk, hs * ns, ns, fs, fs]
        sems = [pltpu.SemaphoreType.DMA((n,)) for n in pairs for _ in range(2)]
        hbm = pl.BlockSpec(memory_space=pl.ANY)
        res = pl.pallas_call(
            functools.partial(kernel, chips, nk),
            out_shape=pltpu.VMEM(signal.shape, BF),
            in_specs=[hbm] * 3,
            out_specs=pl.BlockSpec(memory_space=pltpu.VMEM),
            scratch_shapes=[
                buf, half, half, half, half, buf,
                pltpu.VMEM((2 * st, nb // fold, two, br, LANES), BF),
                pltpu.VMEM((2, nk, chips, 2, no, two, br, LANES), BF),
                pltpu.VMEM((2, two, br, br, nb), BF),
                pltpu.VMEM((br, nb // fold, two * LANES), BF),
                pltpu.VMEM((nb, nb), BF),
                pltpu.VMEM((nb // fold, nb), BF),
                *sems,
                pltpu.SemaphoreType.DMA((3 * nk,)),
                pltpu.SemaphoreType.DMA((2,)),
                pltpu.SemaphoreType.DMA(((2 * hs + 1) * nk,)),
            ],
            compiler_params=pltpu.CompilerParams(
                collective_id=0, has_side_effects=True, vmem_limit_bytes=56 * 2**20
            ),
        )(signal, w1, w2)
        return res.reshape(rows, cols)

    row_spec = P(("dp", "sp"), None)
    weight_spec = P(None, "sp", None, None, None)
    return jax.shard_map(device_program, mesh=mesh, in_specs=(row_spec, weight_spec, weight_spec), out_specs=row_spec, check_vma=False)
```
